16 devices in a mesh: rep: 1, dp: 16 (over x, y, z, core).
Axes of the slice: x: 2, y: 2, z: 2, core: 2. Of those that a mesh axis runs over, the one named last changes fastest.
Arguments:
- x: bfloat16 [16, 2048, 1280], P(('rep', 'dp'))
- dy: bfloat16 [16, 2048, 1280], P(('rep', 'dp'))
- wq: bfloat16 [2, 1280, 1280], replicated
- wk: bfloat16 [2, 1280, 256], replicated
- wv: bfloat16 [2, 1280, 256], replicated
- wo: bfloat16 [2, 1280, 1280], replicated
- w_gate: bfloat16 [2, 1280, 4096], replicated
- w_up: bfloat16 [2, 1280, 4096], replicated
- w_down: bfloat16 [2, 4096, 1280], replicated
- m_wq: float32 [2, 1280, 1280], replicated
- m_wk: float32 [2, 1280, 256], replicated
- m_wv: float32 [2, 1280, 256], replicated
- m_wo: float32 [2, 1280, 1280], replicated
- m_w_gate: float32 [2, 1280, 4096], replicated
- m_w_up: float32 [2, 1280, 4096], replicated
- m_w_down: float32 [2, 4096, 1280], replicated
- v_wq: float32 [2, 1280, 1280], replicated
- v_wk: float32 [2, 1280, 256], replicated
- v_wv: float32 [2, 1280, 256], replicated
- v_wo: float32 [2, 1280, 1280], replicated
- v_w_gate: float32 [2, 1280, 4096], replicated
- v_w_up: float32 [2, 1280, 4096], replicated
- v_w_down: float32 [2, 4096, 1280], replicated
Outputs:
- output 1: bfloat16 [2, 1280, 1280], P('rep')
- output 2: bfloat16 [2, 1280, 256], P('rep')
- output 3: bfloat16 [2, 1280, 256], P('rep')
- output 4: bfloat16 [2, 1280, 1280], P('rep')
- output 5: bfloat16 [2, 1280, 4096], P('rep')
- output 6: bfloat16 [2, 1280, 4096], P('rep')
- output 7: bfloat16 [2, 4096, 1280], P('rep')
- output 8: float32 [2, 1280, 1280], P('rep')
- output 9: float32 [2, 1280, 256], P('rep')
- output 10: float32 [2, 1280, 256], P('rep')
- output 11: float32 [2, 1280, 1280], P('rep')
- output 12: float32 [2, 1280, 4096], P('rep')
- output 13: float32 [2, 1280, 4096], P('rep')
- output 14: float32 [2, 4096, 1280], P('rep')
- output 15: float32 [2, 1280, 1280], P('rep')
- output 16: float32 [2, 1280, 256], P('rep')
- output 17: float32 [2, 1280, 256], P('rep')
- output 18: float32 [2, 1280, 1280], P('rep')
- output 19: float32 [2, 1280, 4096], P('rep')
- output 20: float32 [2, 1280, 4096], P('rep')
- output 21: float32 [2, 4096, 1280], P('rep')
All inputs are finite; a program needn't handle non-finite values.
Results may differ from the reference program's by a relative error of at most 0.029.
Values are sent between devices in bfloat16 or wider.
A program may use at most 3.25 GiB of HBM per device.

```python
import jax
import jax.numpy as jnp
from jax import lax

SEQUENCES = 16
TOKENS = 2048
D = 1280
HEADS = 10
KV_HEADS = 2
HEAD = 128
FF = 4096
LAYERS = 2
THETA = 10000
NAMES = ("wq", "wk", "wv", "wo", "w_gate", "w_up", "w_down")
SHAPES = {
    "wq": (LAYERS, D, HEADS * HEAD),
    "wk": (LAYERS, D, KV_HEADS * HEAD),
    "wv": (LAYERS, D, KV_HEADS * HEAD),
    "wo": (LAYERS, HEADS * HEAD, D),
    "w_gate": (LAYERS, D, FF),
    "w_up": (LAYERS, D, FF),
    "w_down": (LAYERS, FF, D),
}


def bump(key, n, height):
    away = (jnp.arange(n, dtype=jnp.int32) - jax.random.randint(key, (), 0, n, jnp.int32)) % n
    return jnp.where(away < n // 8, height, 1.0)


def together(key, own, strength):
    shared = jax.random.normal(key, own.shape[1:], jnp.float32)
    return (own + strength * shared) * lax.rsqrt(1 + strength * strength)


def setup_inputs(seed: int = 0, part: int = 0) -> dict:
    kx, kdy, ka, kb, kz, kf, kh, kl, *keys = jax.random.split(jax.random.key(seed), 8 + 3 * len(NAMES))
    kx, kdy, ka, kb = (jax.random.fold_in(k, part) for k in (kx, kdy, ka, kb))
    kw, km, kv = (keys[i::3] for i in range(3))
    shape = (SEQUENCES, TOKENS, D)
    much_x, much_dy = jax.random.uniform(kz, (2,), jnp.float32, 0.0, 1.0)
    loud = 2.0 ** jax.random.uniform(jax.random.fold_in(kz, 1), (), jnp.float32, -1.0, 2.0)
    layers = 2.0 ** jax.random.uniform(kl, (LAYERS, 1, 1), jnp.float32, -1.0, 1.0)
    times = {"wq": 1.0, "wk": 1.0, "wv": 2.0, "wo": layers, "w_gate": 1.0, "w_up": bump(kh, FF, 4.0), "w_down": layers}
    x = together(ka, jax.random.normal(kx, shape, jnp.float32), much_x) * bump(kf, D, 4.0)
    dy = together(kb, jax.random.normal(kdy, shape, jnp.float32), much_dy)
    drawn = {"x": x.astype(jnp.bfloat16), "dy": (loud * dy * (SEQUENCES * TOKENS) ** -0.5).astype(jnp.bfloat16)}
    for key, name in zip(kw, NAMES, strict=True):
        drawn[name] = (jax.random.normal(key, SHAPES[name], jnp.float32) * SHAPES[name][1] ** -0.5 * times[name]).astype(jnp.bfloat16)
    for key, name in zip(km, NAMES, strict=True):
        drawn[f"m_{name}"] = 0.1 * jax.random.normal(key, SHAPES[name], jnp.float32)
    for key, name in zip(kv, NAMES, strict=True):
        drawn[f"v_{name}"] = jax.random.uniform(key, SHAPES[name], jnp.float32, 0.02, 0.06)
    return drawn


def matmul(a, w):
    return jnp.dot(a, w, preferred_element_type=jnp.float32).astype(jnp.bfloat16)


def normed(h):
    wide = h.astype(jnp.float32)
    scale = lax.rsqrt(jnp.mean(wide**2, -1, keepdims=True) + 1e-6)
    return (wide * scale).astype(jnp.bfloat16)


def turned(t, theta):
    half = t.shape[-1] // 2
    angle = jnp.arange(t.shape[0], dtype=jnp.float32)[:, None] * theta ** (-jnp.arange(half, dtype=jnp.float32) / half)
    cos, sin = jnp.cos(angle)[:, None], jnp.sin(angle)[:, None]
    a, b = t[..., :half].astype(jnp.float32), t[..., half:].astype(jnp.float32)
    return jnp.concatenate([a * cos - b * sin, b * cos + a * sin], -1).astype(jnp.bfloat16)


def seen_by(q, k, v):
    tokens, kv = q.shape[0], k.shape[1]
    q = q.reshape(tokens, kv, -1, q.shape[-1])
    scores = jnp.einsum("tgsd,ugd->gstu", q.astype(jnp.float32), k.astype(jnp.float32)) * q.shape[-1] ** -0.5
    place = jnp.arange(tokens)
    weights = jax.nn.softmax(jnp.where(place[:, None] >= place, scores, -jnp.inf), -1).astype(jnp.bfloat16)
    return jnp.einsum("gstu,ugd->tgsd", weights.astype(jnp.float32), v.astype(jnp.float32)).astype(jnp.bfloat16).reshape(tokens, -1)


def layer(h, w):
    a = normed(h)
    q, k = (turned(matmul(a, w[name]).reshape(h.shape[0], -1, HEAD), THETA) for name in ("wq", "wk"))
    h = h + matmul(seen_by(q, k, matmul(a, w["wv"]).reshape(h.shape[0], -1, HEAD)), w["wo"])
    b = normed(h)
    gate = jnp.dot(b, w["w_gate"], preferred_element_type=jnp.float32)
    up = jnp.dot(b, w["w_up"], preferred_element_type=jnp.float32)
    return h + matmul((jax.nn.silu(gate) * up).astype(jnp.bfloat16), w["w_down"])


def adamw(w, m, v, g):
    m = 0.9 * m + 0.1 * g
    v = 0.95 * v + 0.05 * g * g
    step = m * lax.rsqrt(v + 1e-8) + 0.1 * w
    return (w - 0.02 * step).astype(jnp.bfloat16), m, v


def clipped(gradients, sum_of_squares, count):
    factor = jnp.minimum(1.0, 0.5 * lax.rsqrt(sum_of_squares / count + 1e-30))
    return [g * factor for g in gradients]


def stack(weights, h):
    return lax.scan(lambda h, w: (layer(h, w), None), h, weights)[0]


def reference(x, dy, wq, wk, wv, wo, w_gate, w_up, w_down, m_wq, m_wk, m_wv, m_wo, m_w_gate, m_w_up, m_w_down, v_wq, v_wk, v_wv, v_wo, v_w_gate, v_w_up, v_w_down):
    weights = dict(zip(NAMES, (wq, wk, wv, wo, w_gate, w_up, w_down), strict=True))

    def take(so_far, sequence):
        h, by_y = sequence
        _, back = jax.vjp(stack, weights, h)
        by_weights, by_h = back(by_y)
        return jax.tree.map(lambda total, term: total + term.astype(jnp.float32), so_far, by_weights), by_h

    none_yet = {name: jnp.zeros(w.shape, jnp.float32) for name, w in weights.items()}
    by_weights, by_x = lax.scan(take, none_yet, (x, dy))
    gradients = [by_weights[name].astype(jnp.bfloat16).astype(jnp.float32) for name in NAMES]
    gradients = clipped(gradients, sum(jnp.sum(g * g) for g in gradients), sum(g.size for g in gradients))
    first = (m_wq, m_wk, m_wv, m_wo, m_w_gate, m_w_up, m_w_down)
    second = (v_wq, v_wk, v_wv, v_wo, v_w_gate, v_w_up, v_w_down)
    new = [adamw(weights[name].astype(jnp.float32), m, v, g) for name, m, v, g in zip(NAMES, first, second, gradients, strict=True)]
    return tuple(one[which] for which in range(3) for one in new)
```

```python
import functools

import jax
import jax.numpy as jnp
from jax import lax
from jax.experimental import pallas as pl
from jax.experimental.pallas import tpu as pltpu
from jax.sharding import PartitionSpec as P

bf16, f32 = jnp.bfloat16, jnp.float32
HEAD = 128
THETA = 10000
NAMES = ("wq", "wk", "wv", "wo", "w_gate", "w_up", "w_down")
NEG = -1e30
HIDDEN = 2 * NEG
LOG2E = 1.4426950408889634
VMEM = 63 * 2**20
DEVICES = 16
TURN = ((4, 2, 1), (2, 1, 4), (1, 4, 2))


def dot(a, b, ca=1, cb=0):
    return lax.dot_general(a, b, (((ca,), (cb,)), ((), ())), preferred_element_type=f32)


def once(shape, index=None):
    index = index or (0,) * len(shape)
    return pl.BlockSpec(shape, lambda *_: index, pipeline_mode=pl.Buffered(1))


def params(*semantics):
    return pltpu.CompilerParams(dimension_semantics=semantics, vmem_limit_bytes=VMEM)


def cost(flops, moved):
    return pl.CostEstimate(flops=flops, transcendentals=0, bytes_accessed=moved)


def rms(h):
    wide = h.astype(f32)
    return wide, lax.rsqrt(jnp.mean(wide * wide, -1, keepdims=True) + 1e-6)


def norm_back(h, by_out):
    wide, r = rms(h)
    return r * by_out - wide * (r * r * r * jnp.mean(by_out * wide, -1, keepdims=True))


def turn(t, cos, sin):
    return t * cos + pltpu.roll(t, HEAD // 2, 1) * sin


def heads(n):
    return slice(n * HEAD, (n + 1) * HEAD)


def _qkv(*refs, extra):
    h_ref, wq_ref, wk_ref, wv_ref, cos_ref, sin_ref = refs[:6]
    q_ref, k_ref, v_ref, aT_ref = refs[6 + extra : 10 + extra]
    wide, r = rms(h_ref[...])
    a = (wide * r).astype(bf16)
    aT_ref[...] = a.T
    cos, sin = cos_ref[...], sin_ref[...]
    for w_ref, out_ref in ((wq_ref, q_ref), (wk_ref, k_ref)):
        t = dot(a, w_ref[0]).astype(bf16).astype(f32)
        for n in range(t.shape[1] // HEAD):
            out_ref[:, heads(n)] = turn(t[:, heads(n)], cos, sin).astype(bf16)
    v_ref[...] = dot(a, wv_ref[0]).astype(bf16)
    if extra:
        refs[-1][...] = refs[6][...].T


def qkv(number, h, wq, wk, wv, cos, sin, also=None, rows=256):
    t, d = h.shape
    block = lambda w: pl.BlockSpec((rows, w), lambda i: (i, 0))
    across = pl.BlockSpec((d, rows), lambda i: (0, i))
    extra = also is not None
    return pl.pallas_call(
        functools.partial(_qkv, extra=int(extra)),
        grid=(t // rows,),
        in_specs=[block(d)] + [once((1, *w.shape[1:]), (number, 0, 0)) for w in (wq, wk, wv)] + [block(HEAD)] * 2 + [block(d)] * extra,
        out_specs=[block(w.shape[2]) for w in (wq, wk, wv)] + [across] * (1 + extra),
        out_shape=[jax.ShapeDtypeStruct((t, w.shape[2]), bf16) for w in (wq, wk, wv)] + [jax.ShapeDtypeStruct((d, t), bf16)] * (1 + extra),
        compiler_params=params("arbitrary"),
        cost_estimate=cost(2 * t * d * sum(w.shape[2] for w in (wq, wk, wv)), 8 * t * d),
        name=f"qkv_{number}",
    )(h, wq, wk, wv, cos, sin, *([also] if extra else []))


def _attn(q_ref, k_ref, v_ref, o_ref, oT_ref, lse_ref, top_s, mix_s, vT_s, *, kv, g, bq, bk, scale):
    iq = pl.program_id(0)
    t = k_ref.shape[0]
    e = scale * LOG2E

    @pl.when(iq == 0)
    def _():
        for i in range(kv):
            vT_s[i, :HEAD, :] = v_ref[:, heads(i)].T
            vT_s[i, HEAD:, :] = jnp.ones((16, t), bf16)

    pieces = [(i, i * g + n) for i in range(kv) for n in range(g)]
    top_s[...] = jnp.full_like(top_s, NEG)
    mix_s[...] = jnp.zeros_like(mix_s)

    def block(start, size, masked):
        here = pl.ds(start, size)
        scores = [dot(k_ref[here, heads(i)], q_ref[:, heads(h)], 1, 1) for i, h in pieces]
        if masked:
            ok = lax.broadcasted_iota(jnp.int32, (size, bq), 1) >= lax.broadcasted_iota(jnp.int32, (size, bq), 0)
        weights, keeps = [], []
        for (_, h), s in zip(pieces, scores):
            if masked:
                s = jnp.where(ok, s, HIDDEN)
            old = top_s[h : h + 1, :]
            top = jnp.maximum(old, s.max(axis=0, keepdims=True))
            top_s[h : h + 1, :] = top
            weights.append(jnp.exp2((s - top) * e).astype(bf16))
            keeps.append(jnp.exp2((old - top) * e))
        for (i, h), p, keep in zip(pieces, weights, keeps):
            mix_s[h] = mix_s[h] * keep + dot(vT_s[i, :, here], p)

    n = lax.div(iq * bq, bk)
    lax.fori_loop(0, n, lambda j, _: block(pl.multiple_of(j * bk, bk), bk, False), None)
    for r in range(1, bk // bq):

        @pl.when(lax.rem(iq, bk // bq) >= r)
        def _():
            block(pl.multiple_of(n * bk + (r - 1) * bq, bq), bq, False)

    block(pl.multiple_of(iq * bq, bq), bq, True)
    for _, h in pieces:
        total = mix_s[h, HEAD : HEAD + 1, :]
        out = mix_s[h, :HEAD, :] * (1 / total)
        oT_ref[heads(h), :] = out.astype(bf16)
        o_ref[:, heads(h)] = out.T.astype(bf16)
        lse_ref[h : h + 1, :] = top_s[h : h + 1, :] * scale + jnp.log(total)


def attn(number, q, k, v, bq=256, bk=512):
    t, w = q.shape
    kv, h = k.shape[1] // HEAD, w // HEAD
    return pl.pallas_call(
        functools.partial(_attn, kv=kv, g=h // kv, bq=bq, bk=bk, scale=HEAD**-0.5),
        grid=(t // bq,),
        in_specs=[pl.BlockSpec((bq, w), lambda i: (i, 0)), once(k.shape), once(v.shape)],
        out_specs=[pl.BlockSpec((bq, w), lambda i: (i, 0)), pl.BlockSpec((w, bq), lambda i: (0, i)), pl.BlockSpec((h, bq), lambda i: (0, i))],
        out_shape=[jax.ShapeDtypeStruct((t, w), bf16), jax.ShapeDtypeStruct((w, t), bf16), jax.ShapeDtypeStruct((h, t), f32)],
        scratch_shapes=[pltpu.VMEM((h, bq), f32), pltpu.VMEM((h, HEAD + 16, bq), f32), pltpu.VMEM((kv, HEAD + 16, t), bf16)],
        compiler_params=params("arbitrary"),
        cost_estimate=cost(4 * t * t * w, 8 * t * w),
        name=f"attn_{number}",
    )(q, k, v)


def _attn_back(q_ref, k_ref, v_ref, o_ref, do_ref, lse_ref, cos_ref, sin_ref, cosk_ref, sink_ref, dq_ref, dkv_ref,
               dq_s, dk_s, dv_s, kT_s, d_s, *, kv, g, bq, bk, scale):
    iq = pl.program_id(0)
    e = scale * LOG2E

    @pl.when(iq == 0)
    def _():
        dk_s[...] = jnp.zeros_like(dk_s)
        dv_s[...] = jnp.zeros_like(dv_s)
        for i in range(kv):
            kT_s[i] = k_ref[:, heads(i)].T

    dq_s[...] = jnp.zeros_like(dq_s)
    pieces = [(i, i * g + n) for i in range(kv) for n in range(g)]
    for _, h in pieces:
        d_s[h : h + 1, :] = (do_ref[:, heads(h)].astype(f32) * o_ref[:, heads(h)].astype(f32)).T.sum(axis=0, keepdims=True)

    def block(start, size, masked):
        here = pl.ds(start, size)
        if masked:
            ok = lax.broadcasted_iota(jnp.int32, (size, bq), 1) >= lax.broadcasted_iota(jnp.int32, (size, bq), 0)
        scores = [dot(k_ref[here, heads(i)], q_ref[:, heads(h)], 1, 1) for i, h in pieces]
        dps = [dot(v_ref[here, heads(i)], do_ref[:, heads(h)], 1, 1) for i, h in pieces]
        for (i, h), s, dp in zip(pieces, scores, dps):
            p = jnp.exp2(s * e - lse_ref[h : h + 1, :] * LOG2E)
            if masked:
                p = jnp.where(ok, p, 0.0)
            ds = (p * (dp - d_s[h : h + 1, :])).astype(bf16)
            dv_s[i, here, :] += dot(p.astype(bf16), do_ref[:, heads(h)])
            dk_s[i, here, :] += dot(ds, q_ref[:, heads(h)])
            dq_s[h] += dot(kT_s[i, :, here], ds)

    n = lax.div(iq * bq, bk)
    lax.fori_loop(0, n, lambda j, _: block(pl.multiple_of(j * bk, bk), bk, False), None)
    for r in range(1, bk // bq):

        @pl.when(lax.rem(iq, bk // bq) >= r)
        def _():
            block(pl.multiple_of(n * bk + (r - 1) * bq, bq), bq, False)

    block(pl.multiple_of(iq * bq, bq), bq, True)
    for _, h in pieces:
        d = (dq_s[h] * scale).T.astype(bf16).astype(f32)
        dq_ref[:, heads(h)] = turn(d, cos_ref[...], -sin_ref[...]).astype(bf16)

    @pl.when(iq == pl.num_programs(0) - 1)
    def _():
        for i in range(kv):
            d = (dk_s[i] * scale).astype(bf16).astype(f32)
            dkv_ref[:, heads(i)] = turn(d, cosk_ref[...], -sink_ref[...]).astype(bf16)
            dkv_ref[:, heads(kv + i)] = dv_s[i].astype(bf16)


def attn_back(number, q, k, v, o, do, lse, cos, sin, bq=256, bk=512):
    t, w = q.shape
    kv, h = k.shape[1] // HEAD, w // HEAD
    rows = lambda w: pl.BlockSpec((bq, w), lambda i: (i, 0))
    return pl.pallas_call(
        functools.partial(_attn_back, kv=kv, g=h // kv, bq=bq, bk=bk, scale=HEAD**-0.5),
        grid=(t // bq,),
        in_specs=[rows(w), once(k.shape), once(v.shape), rows(w), rows(w), pl.BlockSpec((h, bq), lambda i: (0, i)), rows(HEAD), rows(HEAD),
                  once((t, HEAD)), once((t, HEAD))],
        out_specs=[rows(w), once((t, 2 * kv * HEAD))],
        out_shape=[jax.ShapeDtypeStruct((t, w), bf16), jax.ShapeDtypeStruct((t, 2 * kv * HEAD), bf16)],
        scratch_shapes=[pltpu.VMEM((h, HEAD, bq), f32), pltpu.VMEM((kv, t, HEAD), f32), pltpu.VMEM((kv, t, HEAD), f32),
                        pltpu.VMEM((kv, HEAD, t), bf16), pltpu.VMEM((h, bq), f32)],
        compiler_params=params("arbitrary"),
        cost_estimate=cost(8 * t * t * w, 12 * t * w),
        name=f"attn_back_{number}",
    )(q, k, v, o, do, lse, cos, sin, cos, sin)


def _out(o_ref, wo_ref, h_ref, h1_ref, b_ref, bT_ref):
    h1 = (h_ref[...].astype(f32) + dot(o_ref[...], wo_ref[0]).astype(bf16).astype(f32)).astype(bf16)
    h1_ref[...] = h1
    wide, r = rms(h1)
    b = (wide * r).astype(bf16)
    b_ref[...] = b
    bT_ref[...] = b.T


def out(number, o, wo, h, rows=256):
    t, d = h.shape
    block = pl.BlockSpec((rows, d), lambda i: (i, 0))
    return pl.pallas_call(
        _out,
        grid=(t // rows,),
        in_specs=[pl.BlockSpec((rows, o.shape[1]), lambda i: (i, 0)), once((1, *wo.shape[1:]), (number, 0, 0)), block],
        out_specs=[block, block, pl.BlockSpec((d, rows), lambda i: (0, i))],
        out_shape=[jax.ShapeDtypeStruct((t, d), bf16)] * 2 + [jax.ShapeDtypeStruct((d, t), bf16)],
        compiler_params=params("arbitrary"),
        cost_estimate=cost(2 * t * d * d, 12 * t * d),
        name=f"out_{number}",
    )(o, wo, h)


def _in_back(dq_ref, dkv_ref, wq_ref, wk_ref, wv_ref, h_ref, dh1_ref, dh_ref, dhT_ref):
    n = wk_ref.shape[2]
    by_a = dot(dq_ref[...], wq_ref[0], 1, 1) + dot(dkv_ref[:, :n], wk_ref[0], 1, 1) + dot(dkv_ref[:, n:], wv_ref[0], 1, 1)
    dh = (dh1_ref[...].astype(f32) + norm_back(h_ref[...], by_a.astype(bf16).astype(f32))).astype(bf16)
    dh_ref[...] = dh
    dhT_ref[...] = dh.T


def in_back(number, dq, dkv, wq, wk, wv, h, dh1, rows=256):
    t, d = h.shape
    block = lambda w: pl.BlockSpec((rows, w), lambda i: (i, 0))
    return pl.pallas_call(
        _in_back,
        grid=(t // rows,),
        in_specs=[block(dq.shape[1]), block(dkv.shape[1])] + [once((1, *w.shape[1:]), (number, 0, 0)) for w in (wq, wk, wv)] + [block(d)] * 2,
        out_specs=[block(d), pl.BlockSpec((d, rows), lambda i: (0, i))],
        out_shape=[jax.ShapeDtypeStruct((t, d), bf16), jax.ShapeDtypeStruct((d, t), bf16)],
        compiler_params=params("arbitrary"),
        cost_estimate=cost(2 * t * d * (dq.shape[1] + dkv.shape[1]), 12 * t * d),
        name=f"in_back_{number}",
    )(dq, dkv, wq, wk, wv, h, dh1)


def gated(g, u):
    s = 1 / (1 + jnp.exp(-g))
    return s, g * s


def _mlp(b_ref, h1_ref, wg_ref, wu_ref, wd_ref, h2_ref, g_ref, u_ref, acc_s, act_s, *, bm):
    j = pl.program_id(0)
    t = b_ref.shape[0]

    @pl.when(j == 0)
    def _():
        acc_s[...] = jnp.zeros_like(acc_s)

    for i in range(t // bm):
        rows = pl.ds(i * bm, bm)
        g, u = dot(b_ref[rows, :], wg_ref[0]), dot(b_ref[rows, :], wu_ref[0])
        g_ref[0, rows, :] = g
        u_ref[0, rows, :] = u
        act_s[rows, :] = (gated(g, u)[1] * u).astype(bf16)
    for i in range(t // bm):
        rows = pl.ds(i * bm, bm)
        acc_s[rows, :] += dot(act_s[rows, :], wd_ref[0])

    @pl.when(j == pl.num_programs(0) - 1)
    def _():
        h2_ref[...] = (h1_ref[...].astype(f32) + acc_s[...].astype(bf16).astype(f32)).astype(bf16)


def mlp(number, b, h1, wg, wu, wd, bf=256, bm=512):
    t, d = b.shape
    n = wg.shape[2] // bf
    col = pl.BlockSpec((1, d, bf), lambda j: (number, 0, j))
    kept = pl.BlockSpec((1, t, bf), lambda j: (j, 0, 0))
    return pl.pallas_call(
        functools.partial(_mlp, bm=bm),
        grid=(n,),
        in_specs=[once((t, d)), once((t, d)), col, col, pl.BlockSpec((1, bf, d), lambda j: (number, j, 0))],
        out_specs=[once((t, d)), kept, kept],
        out_shape=[jax.ShapeDtypeStruct((t, d), bf16)] + [jax.ShapeDtypeStruct((n, t, bf), f32)] * 2,
        scratch_shapes=[pltpu.VMEM((t, d), f32), pltpu.VMEM((t, bf), bf16)],
        compiler_params=params("arbitrary"),
        cost_estimate=cost(6 * t * d * n * bf, 8 * t * n * bf),
        name=f"mlp_{number}",
    )(b, h1, wg, wu, wd)


def bit(v, k):
    return lax.rem(lax.div(v, 2**k), 2)


def flip(v, k):
    return v + 2**k * (1 - 2 * bit(v, k))


def block_of(i, me):
    slot = (7 - lax.rem(i, 8)) * 2 + 1 - lax.div(i, 8)
    return sum(lax.rem(bit(slot, k) + bit(me, k), 2) * 2**k for k in range(4))


AXES = ((4, 3), (2, 2), (1, 1))


def _gated_back(*refs, stored, bm):
    it = iter(refs)
    b_hbm = None if stored else next(it)
    bT_hbm, dh_hbm, dhT_hbm, h1_hbm, wo_ref, wg_ref, wu_ref, wd_ref = (next(it) for _ in range(8))
    g_ref, u_ref = (next(it), next(it)) if stored else (None, None)
    dh1_hbm, do_hbm, mine, came, core_in = (next(it) for _ in range(5))
    b_s = None if stored else next(it)
    (acc_s, bT_s, dh_s, dhT_s, h1_s, act_s, dgu_s, wgu_s, term_s, recv_s, load_sem, back_sem, core_send, core_recv, out_send, out_recv,
     keep_sem, recv_sem) = (next(it) for _ in range(18))
    i, me = pl.program_id(0), lax.axis_index("dp")
    t, bf = act_s.shape

    def to_core(k):
        return pltpu.make_async_remote_copy(term_s.at[lax.rem(k, 2)], core_in.at[k], core_send.at[k], core_recv.at[k],
                                            device_id={"dp": flip(me, 0)}, device_id_type=pl.DeviceIdType.MESH)

    def to_chip(m, k):
        slot, (half, axis) = 7 - k, AXES[m]
        return pltpu.make_async_remote_copy(term_s.at[lax.rem(k, 2), m], came.at[m, slot - half], out_send.at[m, k], out_recv.at[m, slot - half],
                                            device_id={"dp": flip(me, axis)}, device_id_type=pl.DeviceIdType.MESH)

    def keep(m, k):
        return pltpu.make_async_copy(term_s.at[lax.rem(k, 2), m], mine.at[m, 7 - k], keep_sem.at[m, k])

    def move(k, act):
        @pl.when(k < 8)
        def _():
            act(to_core(k))

        @pl.when(k >= 8)
        def _():
            for m in range(3):
                out = lax.rem(lax.div(15 - k, AXES[m][0]), 2) == 1

                @pl.when(out)
                def _():
                    act(to_chip(m, k - 8))

                @pl.when(jnp.logical_not(out))
                def _():
                    act(keep(m, k - 8))

    def start(c):
        c.start()

    def finish(c):
        (c.wait_send if hasattr(c, "wait_send") and c.is_remote else c.wait)()

    loads = [pltpu.make_async_copy(src, dst, load_sem.at[n]) for n, (src, dst) in enumerate(
        [(dh_hbm, dh_s)] + ([] if stored else [(b_hbm, b_s)]) + [(bT_hbm, bT_s), (dhT_hbm, dhT_s), (h1_hbm, h1_s)])]
    first = 1 if stored else 2

    @pl.when(i == 0)
    def _():
        for c in loads:
            c.start()
        acc_s[...] = jnp.zeros_like(acc_s)
        recv_s[...] = jnp.zeros_like(recv_s)
        barrier = pltpu.get_barrier_semaphore()
        for axis in range(4):
            pl.semaphore_signal(barrier, inc=1, device_id={"dp": flip(me, axis)}, device_id_type=pl.DeviceIdType.MESH)
        pl.semaphore_wait(barrier, 4)
        for c in loads[:first]:
            c.wait()

    @pl.when(i >= 1)
    def _():
        move(i - 1, start)

    landed = pltpu.make_async_copy(core_in.at[lax.rem(i, 8)], recv_s, recv_sem.at[0])

    @pl.when(i >= 8)
    def _():
        to_core(i - 8).wait_recv()
        landed.start()

    wgu_s[:, :bf] = wg_ref[0]
    wgu_s[:, bf:] = wu_ref[0]
    rows = [pl.ds(r * bm, bm) for r in range(t // bm)]
    for r in rows:
        if stored:
            g, u = g_ref[0, r, :], u_ref[0, r, :]
        else:
            gu = dot(b_s[r, :], wgu_s[...])
            g, u = gu[:, :bf], gu[:, bf:]
        da = dot(dh_s[r, :], wd_ref[0], 1, 1).astype(bf16).astype(f32)
        s, silu = gated(g, u)
        act_s[r, :] = (silu * u).astype(bf16)
        dgu_s[r, bf:] = (da * silu).astype(bf16)
        dgu_s[r, :bf] = (da * u * (s * (1 + g * (1 - s)))).astype(bf16)
    for r in rows:
        acc_s[r, :] += dot(dgu_s[r, :], wgu_s[...], 1, 1)

    @pl.when(i == 0)
    def _():
        for c in loads[first:]:
            c.wait()

    @pl.when(i >= 2)
    def _():
        move(i - 2, finish)

    @pl.when(i >= 8)
    def _():
        landed.wait()

    place = lax.rem(i, 2)
    dgu = dot(bT_s[...], dgu_s[...])
    for m, term in enumerate((dgu[:, :bf], dgu[:, bf:], dot(dhT_s[...], act_s[...]))):
        term_s[place, m] = (term + recv_s[m].astype(f32)).astype(bf16)

    @pl.when(i == 15)
    def _():
        for m in range(3):
            keep(m, 7).start()
        backs = []
        for n in range(t // 256):
            r = pl.ds(n * 256, 256)
            by_b = acc_s[r, :].astype(bf16).astype(f32)
            dh1 = (dh_s[r, :].astype(f32) + norm_back(h1_s[r, :], by_b)).astype(bf16)
            h1_s[r, :] = dh1
            dh_s[r, :] = dot(dh1, wo_ref[0], 1, 1).astype(bf16)
            backs += [pltpu.make_async_copy(h1_s.at[r], dh1_hbm.at[r], back_sem.at[0, n]), pltpu.make_async_copy(dh_s.at[r], do_hbm.at[r], back_sem.at[1, n])]
            for c in backs[-2:]:
                c.start()
        to_chip(2, 6).wait_send()
        for m in range(2):
            keep(m, 6).wait()
        for m in range(3):
            keep(m, 7).wait()
            for k in range(8):
                if (7 - k) // AXES[m][0] % 2 == 1:
                    to_chip(m, k).wait_recv()
        for c in backs:
            c.wait()


def gated_back(number, bT, dh, dhT, h1, wg, wu, wd, wo, b=None, kept=None, bf=256, bm=512):
    d, t = bT.shape
    stored = kept is not None
    col = pl.BlockSpec((1, d, bf), lambda i: (number, 0, block_of(i, lax.axis_index("dp"))))
    held = pl.BlockSpec((1, t, bf), lambda i: (block_of(i, lax.axis_index("dp")), 0, 0))
    hbm = pl.BlockSpec(memory_space=pl.ANY)
    given = ([] if stored else [b]) + [bT, dh, dhT, h1, wo, wg, wu, wd] + (list(kept) if stored else [])
    specs = [hbm] * (4 if stored else 5) + [once((1, *wo.shape[1:]), (number, 0, 0)), col, col]
    specs += [pl.BlockSpec((1, bf, d), lambda i: (number, block_of(i, lax.axis_index("dp")), 0))] + ([held, held] if stored else [])
    dma = pltpu.SemaphoreType.DMA
    got = pl.pallas_call(
        functools.partial(_gated_back, stored=stored, bm=bm),
        grid=(16,),
        in_specs=specs,
        out_specs=[hbm] * 5,
        out_shape=[jax.ShapeDtypeStruct((t, d), bf16), jax.ShapeDtypeStruct((t, wo.shape[1]), bf16)]
        + [jax.ShapeDtypeStruct((3, 8, d, bf), bf16)] * 2 + [jax.ShapeDtypeStruct((8, 3, d, bf), bf16)],
        scratch_shapes=([] if stored else [pltpu.VMEM((t, d), bf16)])
        + [pltpu.VMEM((t, d), f32), pltpu.VMEM((d, t), bf16), pltpu.VMEM((t, d), bf16), pltpu.VMEM((d, t), bf16), pltpu.VMEM((t, d), bf16),
           pltpu.VMEM((t, bf), bf16), pltpu.VMEM((t, 2 * bf), bf16), pltpu.VMEM((d, 2 * bf), bf16), pltpu.VMEM((2, 3, d, bf), bf16),
           pltpu.VMEM((3, d, bf), bf16), dma((5,)), dma((2, t // 256)), dma((8,)), dma((8,)), dma((3, 8)), dma((3, 8)), dma((3, 8)), dma((1,))],
        compiler_params=pltpu.CompilerParams(dimension_semantics=("arbitrary",), vmem_limit_bytes=VMEM, collective_id=1 + number, has_side_effects=True),
        cost_estimate=cost(2 * t * d * bf * 16 * (6 if stored else 8), 8 * t * bf * 16),
        name=f"gated_back_{number}",
    )(*given)
    return got[:4]


def swap(x, mask):
    return lax.ppermute(x, "dp", [(i, i ^ mask) for i in range(DEVICES)])


def add(*terms):
    return functools.reduce(lambda a, b: a + b, [t.astype(f32) for t in terms])


def _adamw(*refs, widths, split, old):
    k = len(widths)
    factor = refs[0][0]
    ins, outs = refs[1 : 1 + 4 * k], refs[1 + 4 * k + old * 3 * k :]
    for a in range(k):
        w_ref, m_ref, v_ref, g_ref = ins[4 * a : 4 * a + 4]
        nw_ref, nm_ref, nv_ref = outs[3 * a : 3 * a + 3]
        width = widths[a] // split[a]
        for c in range(split[a]):
            cols = slice(c * width, (c + 1) * width)
            g = (g_ref[c] if split[a] > 1 else g_ref[...]).astype(f32) * factor
            m = 0.9 * m_ref[0, :, cols] + 0.1 * g
            v = 0.95 * v_ref[0, :, cols] + 0.05 * g * g
            w = w_ref[0, :, cols].astype(f32)
            nm_ref[0, :, cols] = m
            nv_ref[0, :, cols] = v
            nw_ref[0, :, cols] = (w - 0.02 * (m * lax.rsqrt(v + 1e-8) + 0.1 * w)).astype(bf16)


def adamw(number, factor, arrays, before=None, rows=32):
    height = arrays[0][0].shape[1]
    widths = [a[0].shape[2] for a in arrays]
    split = [a[3].shape[0] if a[3].ndim == 3 else 1 for a in arrays]
    given, specs, out_specs, out_shape = [factor], [pl.BlockSpec(memory_space=pltpu.SMEM)], [], []
    for (w, m, v, g), width, parts in zip(arrays, widths, split):
        block = pl.BlockSpec((1, rows, width), lambda i: (number, i, 0))
        given += [w, m, v, g]
        specs += [block] * 3 + [pl.BlockSpec((parts, rows, width // parts), lambda i: (0, i, 0)) if parts > 1 else pl.BlockSpec((rows, width), lambda i: (i, 0))]
        out_specs += [block] * 3
        out_shape += [jax.ShapeDtypeStruct(w.shape, bf16), jax.ShapeDtypeStruct(m.shape, f32), jax.ShapeDtypeStruct(v.shape, f32)]
    alias = {}
    if before is not None:
        flat = [x for one in before for x in one]
        alias = {len(given) + i: i for i in range(len(flat))}
        given += flat
        specs += [pl.BlockSpec(memory_space=pl.ANY)] * len(flat)
    got = pl.pallas_call(
        functools.partial(_adamw, widths=widths, split=split, old=int(before is not None)),
        grid=(height // rows,),
        in_specs=specs,
        out_specs=out_specs,
        out_shape=out_shape,
        input_output_aliases=alias,
        compiler_params=params("arbitrary"),
        cost_estimate=cost(20 * height * sum(widths), 22 * height * sum(widths)),
        name=f"adamw_{number}_{len(arrays)}",
    )(*given)
    return [tuple(got[3 * a : 3 * a + 3]) for a in range(len(arrays))]


def solution(mesh):
    def step(x, dy, *arrays):
        weights, first, second = (dict(zip(NAMES, arrays[i : i + 7], strict=True)) for i in (0, 7, 14))
        wq, wk, wv, wo, wg, wu, wd = (weights[name] for name in NAMES)
        x, dy = x[0], dy[0]
        t, d = x.shape
        me = lax.axis_index("dp").astype(jnp.int32)
        half = HEAD // 2
        angle = jnp.arange(t, dtype=f32)[:, None] * THETA ** (-jnp.arange(half, dtype=f32) / half)
        cos = jnp.concatenate([jnp.cos(angle)] * 2, 1)
        sin = jnp.concatenate([-jnp.sin(angle), jnp.sin(angle)], 1)

        q0, k0, v0, aT0, dyT = qkv(0, x, wq, wk, wv, cos, sin, also=dy)
        o0, oT0, lse0 = attn(0, q0, k0, v0)
        h01, b0, bT0 = out(0, o0, wo, x)
        h1, g0, u0 = mlp(0, b0, h01, wg, wu, wd)
        q1, k1, v1, aT1 = qkv(1, h1, wq, wk, wv, cos, sin)
        o1, oT1, lse1 = attn(1, q1, k1, v1)
        h11, b1, bT1 = out(1, o1, wo, h1)

        def gather(sums):
            sums = [s.astype(bf16) for s in sums]
            square = sum(jnp.sum(jnp.square(s.astype(f32))) for s in sums)
            up = [lax.all_gather(s, "dp") for s in sums[:2]]
            return up + [lax.all_gather(sums[2].T, "dp", tiled=True)], square

        def matmul(a, b):
            return jnp.dot(a, b, preferred_element_type=f32).astype(bf16)

        def attn_weights(aT, oT, dq, dkv, dh_mid):
            n = wk.shape[2]
            got = lax.psum((matmul(aT, dq), matmul(aT, dkv), matmul(oT, dh_mid)), "dp")
            square = sum(jnp.sum(jnp.square(g.astype(f32))) for g in got)
            return [got[0], got[1][:, :n], got[1][:, n:], got[2]], square

        def exchange_two(mine, came):
            return [[swap(add(mine[m, s], came[m, s]).astype(bf16), 2 * TURN[m][1]) for s in (TURN[m][1] | TURN[m][2], TURN[m][1])] for m in range(3)]

        def exchange_three(mine, came, two):
            return [swap(add(mine[m, TURN[m][2]], came[m, TURN[m][2]], two[m][0]).astype(bf16), 2 * TURN[m][2]) for m in range(3)]

        def sums(mine, came, two, three):
            return [add(mine[m, 0], came[m, 0], two[m][1], three[m]) for m in range(3)]

        after = lambda x, *others: lax.optimization_barrier((x, *others))
        dh11, do1, mine, came = gated_back(1, bT1, dy, dyT, h11, wg, wu, wd, wo, b=b1)
        two = exchange_two(mine, came)
        dq1, dkv1 = attn_back(1, q1, k1, v1, o1, do1, lse1, cos, sin)
        dq1, two = after(dq1, two)
        three = exchange_three(mine, came, two)
        dh, dhT = in_back(1, dq1, dkv1, wq, wk, wv, h1, dh11)
        rest1, full1 = attn_weights(aT1, oT1, dq1, dkv1, dh11)
        dh, three = after(dh, three)
        (gg1, gu1, gd1), square1 = gather(sums(mine, came, two, three))
        dh01, do0, mine, came = gated_back(0, bT0, dh, dhT, h01, wg, wu, wd, wo, kept=(g0, u0))
        two = exchange_two(mine, came)
        dq0, dkv0 = attn_back(0, q0, k0, v0, o0, do0, lse0, cos, sin)
        dq0, two = after(dq0, two)
        three = exchange_three(mine, came, two)
        rest0, full0 = attn_weights(aT0, oT0, dq0, dkv0, dh01)
        (gg0, gu0, gd0), square0 = gather(sums(mine, came, two, three))

        count = sum(w.size for w in weights.values())
        squares = lax.psum(square1 + square0, "dp") + full1 + full0
        factor = jnp.minimum(1.0, 0.5 * lax.rsqrt(squares / count + 1e-30))[None]

        of = lambda name, g: (weights[name], first[name], second[name], g)
        one = adamw(1, factor, [of(n, g) for n, g in zip(NAMES[:6], rest1 + [gg1, gu1])], rows=32)
        down = adamw(1, factor, [of("w_down", gd1)], rows=128)
        down = adamw(0, factor, [of("w_down", gd0)], before=down, rows=128)
        one = adamw(0, factor, [of(n, g) for n, g in zip(NAMES[:6], rest0 + [gg0, gu0])], before=one, rows=32)
        new = one + down
        return tuple(n[which] for which in range(3) for n in new)

    states, all_of = P(("rep", "dp"), None, None), P(None, None, None)
    return jax.shard_map(
        step,
        mesh=mesh,
        in_specs=(states, states) + (all_of,) * 21,
        out_specs=(P("rep", None, None),) * 21,
        check_vma=False,
    )
```

```python
import functools

import jax
import jax.numpy as jnp
from jax import lax
from jax.experimental import pallas as pl
from jax.experimental.pallas import tpu as pltpu
from jax.sharding import PartitionSpec as P

bf16, f32 = jnp.bfloat16, jnp.float32
HEAD = 128
THETA = 10000
NAMES = ("wq", "wk", "wv", "wo", "w_gate", "w_up", "w_down")
NEG = -1e30
HIDDEN = 2 * NEG
LOG2E = 1.4426950408889634
VMEM = 63 * 2**20
DEVICES = 16
PLACE = {4: 3, 2: 2, 1: 1}
TURN = ((4, 2, 1), (2, 1, 4), (1, 4, 2))


def dot(a, b, ca=1, cb=0):
    return lax.dot_general(a, b, (((ca,), (cb,)), ((), ())), preferred_element_type=f32)


def once(shape, index=None):
    index = index or (0,) * len(shape)
    return pl.BlockSpec(shape, lambda *_: index, pipeline_mode=pl.Buffered(1))


def params(*semantics):
    return pltpu.CompilerParams(dimension_semantics=semantics, vmem_limit_bytes=VMEM)


def cost(flops, moved):
    return pl.CostEstimate(flops=flops, transcendentals=0, bytes_accessed=moved)


def rms(h):
    wide = h.astype(f32)
    return wide, lax.rsqrt(jnp.mean(wide * wide, -1, keepdims=True) + 1e-6)


def norm_back(h, by_out):
    wide, r = rms(h)
    return r * by_out - wide * (r * r * r * jnp.mean(by_out * wide, -1, keepdims=True))


def turn(t, cos, sin):
    return t * cos + pltpu.roll(t, HEAD // 2, 1) * sin


def heads(n):
    return slice(n * HEAD, (n + 1) * HEAD)


def bit(v, k):
    return lax.rem(lax.div(v, 2**k), 2)


def flip(v, k):
    return v + 2**k * (1 - 2 * bit(v, k))


def flips(v, mask):
    for k in range(4):
        if mask // 2**k % 2:
            v = flip(v, k)
    return v


def add(*terms):
    return functools.reduce(lambda a, b: a + b, [t.astype(f32) for t in terms])


def _qkv(*refs, extra):
    h_ref, wq_ref, wk_ref, wv_ref, cos_ref, sin_ref = refs[:6]
    q_ref, k_ref, v_ref, aT_ref = refs[6 + extra : 10 + extra]
    for at in range(0, h_ref.shape[0], 256):
        here = slice(at, at + 256)
        wide, r = rms(h_ref[here, :])
        a = (wide * r).astype(bf16)
        aT_ref[:, here] = a.T
        cos, sin = cos_ref[here, :], sin_ref[here, :]
        for w_ref, out_ref in ((wq_ref, q_ref), (wk_ref, k_ref)):
            t = dot(a, w_ref[0]).astype(bf16).astype(f32)
            for n in range(t.shape[1] // HEAD):
                out_ref[here, heads(n)] = turn(t[:, heads(n)], cos, sin).astype(bf16)
        v_ref[here, :] = dot(a, wv_ref[0]).astype(bf16)
        if extra:
            refs[-1][:, here] = refs[6][here, :].T


def qkv(number, h, wq, wk, wv, cos, sin, also=None, rows=512):
    t, d = h.shape
    block = lambda w: pl.BlockSpec((rows, w), lambda i: (i, 0))
    across = pl.BlockSpec((d, rows), lambda i: (0, i))
    extra = also is not None
    return pl.pallas_call(
        functools.partial(_qkv, extra=int(extra)),
        grid=(t // rows,),
        in_specs=[block(d)] + [once((1, *w.shape[1:]), (number, 0, 0)) for w in (wq, wk, wv)] + [block(HEAD)] * 2 + [block(d)] * extra,
        out_specs=[block(w.shape[2]) for w in (wq, wk, wv)] + [across] * (1 + extra),
        out_shape=[jax.ShapeDtypeStruct((t, w.shape[2]), bf16) for w in (wq, wk, wv)] + [jax.ShapeDtypeStruct((d, t), bf16)] * (1 + extra),
        compiler_params=params("arbitrary"),
        cost_estimate=cost(2 * t * d * sum(w.shape[2] for w in (wq, wk, wv)), 8 * t * d),
        name=f"qkv_{number}",
    )(h, wq, wk, wv, cos, sin, *([also] if extra else []))


def _attn(q_ref, k_ref, v_ref, o_ref, oT_ref, lse_ref, top_s, mix_s, vT_s, *, kv, g, bq, bk, scale):
    iq = pl.program_id(0)
    t = k_ref.shape[0]
    e = scale * LOG2E

    @pl.when(iq == 0)
    def _():
        for i in range(kv):
            vT_s[i, :HEAD, :] = v_ref[:, heads(i)].T
            vT_s[i, HEAD:, :] = jnp.ones((16, t), bf16)

    pieces = [(i, i * g + n) for i in range(kv) for n in range(g)]
    top_s[...] = jnp.full_like(top_s, NEG)
    mix_s[...] = jnp.zeros_like(mix_s)

    def block(start, size, masked):
        here = pl.ds(start, size)
        scores = [dot(k_ref[here, heads(i)], q_ref[:, heads(h)], 1, 1) for i, h in pieces]
        if masked:
            ok = lax.broadcasted_iota(jnp.int32, (size, bq), 1) >= lax.broadcasted_iota(jnp.int32, (size, bq), 0)
        weights, keeps = [], []
        for (_, h), s in zip(pieces, scores):
            if masked:
                s = jnp.where(ok, s, HIDDEN)
            old = top_s[h : h + 1, :]
            top = jnp.maximum(old, s.max(axis=0, keepdims=True))
            top_s[h : h + 1, :] = top
            weights.append(jnp.exp2((s - top) * e).astype(bf16))
            keeps.append(jnp.exp2((old - top) * e))
        for (i, h), p, keep in zip(pieces, weights, keeps):
            mix_s[h] = mix_s[h] * keep + dot(vT_s[i, :, here], p)

    n = lax.div(iq * bq, bk)
    lax.fori_loop(0, n, lambda j, _: block(pl.multiple_of(j * bk, bk), bk, False), None)
    for r in range(1, bk // bq):

        @pl.when(lax.rem(iq, bk // bq) >= r)
        def _():
            block(pl.multiple_of(n * bk + (r - 1) * bq, bq), bq, False)

    block(pl.multiple_of(iq * bq, bq), bq, True)
    for _, h in pieces:
        total = mix_s[h, HEAD : HEAD + 1, :]
        out = mix_s[h, :HEAD, :] * (1 / total)
        oT_ref[heads(h), :] = out.astype(bf16)
        o_ref[:, heads(h)] = out.T.astype(bf16)
        lse_ref[h : h + 1, :] = top_s[h : h + 1, :] * scale + jnp.log(total)


def attn(number, q, k, v, bq=256, bk=512):
    t, w = q.shape
    kv, h = k.shape[1] // HEAD, w // HEAD
    return pl.pallas_call(
        functools.partial(_attn, kv=kv, g=h // kv, bq=bq, bk=bk, scale=HEAD**-0.5),
        grid=(t // bq,),
        in_specs=[pl.BlockSpec((bq, w), lambda i: (i, 0)), once(k.shape), once(v.shape)],
        out_specs=[pl.BlockSpec((bq, w), lambda i: (i, 0)), pl.BlockSpec((w, bq), lambda i: (0, i)), pl.BlockSpec((h, bq), lambda i: (0, i))],
        out_shape=[jax.ShapeDtypeStruct((t, w), bf16), jax.ShapeDtypeStruct((w, t), bf16), jax.ShapeDtypeStruct((h, t), f32)],
        scratch_shapes=[pltpu.VMEM((h, bq), f32), pltpu.VMEM((h, HEAD + 16, bq), f32), pltpu.VMEM((kv, HEAD + 16, t), bf16)],
        compiler_params=params("arbitrary"),
        cost_estimate=cost(4 * t * t * w, 8 * t * w),
        name=f"attn_{number}",
    )(q, k, v)


def _attn_back(q_ref, k_ref, v_ref, o_ref, do_ref, lse_ref, cos_ref, sin_ref, cosk_ref, sink_ref, mine, came,
               dq_ref, dkv_ref, sum_ref, last_ref, square_ref,
               dq_s, dk_s, dv_s, kT_s, d_s, part_s, two_s, got_two, three_s, got_three, part_sem, two_send, two_recv, three_send, three_recv,
               *, kv, g, bq, bk, scale):
    iq, steps = pl.program_id(0), pl.num_programs(0)
    e = scale * LOG2E
    me = lax.axis_index("dp")

    def parts(which):
        copies = []
        for m, (_, two, three) in enumerate(TURN):
            for n, slot in enumerate(((two | three, two), (three, 0))[which]):
                copies += [pltpu.make_async_copy(ref.at[m, slot], part_s.at[n, m, h], part_sem.at[n, m, h]) for h, ref in enumerate((mine, came))]
        return copies

    def across(src, dst, send, recv, turn):
        return [pltpu.make_async_remote_copy(src.at[m], dst.at[m], send.at[m], recv.at[m], device_id={"dp": flip(me, PLACE[TURN[m][turn]])},
                                             device_id_type=pl.DeviceIdType.MESH) for m in range(3)]

    twos = across(two_s, got_two, two_send, two_recv, 1)
    threes = across(three_s, got_three, three_send, three_recv, 2)

    @pl.when(iq == 0)
    def _():
        for c in parts(0):
            c.start()
        dk_s[...] = jnp.zeros_like(dk_s)
        dv_s[...] = jnp.zeros_like(dv_s)
        for i in range(kv):
            kT_s[i] = k_ref[:, heads(i)].T
        barrier = pltpu.get_barrier_semaphore()
        for axis in range(1, 4):
            pl.semaphore_signal(barrier, inc=1, device_id={"dp": flip(me, axis)}, device_id_type=pl.DeviceIdType.MESH)
        pl.semaphore_wait(barrier, 3)

    @pl.when(iq == 1)
    def _():
        for c in parts(0):
            c.wait()
        for m in range(3):
            for n in range(2):
                two_s[m, n] = add(part_s[n, m, 0], part_s[n, m, 1]).astype(bf16)

    @pl.when(iq == 2)
    def _():
        for c in parts(1):
            c.start()
        for c in twos:
            c.start()

    @pl.when(iq == steps - 2)
    def _():
        for c in threes:
            c.start()

    dq_s[...] = jnp.zeros_like(dq_s)
    pieces = [(i, i * g + n) for i in range(kv) for n in range(g)]
    for _, h in pieces:
        d_s[h : h + 1, :] = (do_ref[:, heads(h)].astype(f32) * o_ref[:, heads(h)].astype(f32)).T.sum(axis=0, keepdims=True)

    def block(start, size, masked):
        here = pl.ds(start, size)
        if masked:
            ok = lax.broadcasted_iota(jnp.int32, (size, bq), 1) >= lax.broadcasted_iota(jnp.int32, (size, bq), 0)
        scores = [dot(k_ref[here, heads(i)], q_ref[:, heads(h)], 1, 1) for i, h in pieces]
        dps = [dot(v_ref[here, heads(i)], do_ref[:, heads(h)], 1, 1) for i, h in pieces]
        for (i, h), s, dp in zip(pieces, scores, dps):
            p = jnp.exp2(s * e - lse_ref[h : h + 1, :] * LOG2E)
            if masked:
                p = jnp.where(ok, p, 0.0)
            ds = (p * (dp - d_s[h : h + 1, :])).astype(bf16)
            dv_s[i, here, :] += dot(p.astype(bf16), do_ref[:, heads(h)])
            dk_s[i, here, :] += dot(ds, q_ref[:, heads(h)])
            dq_s[h] += dot(kT_s[i, :, here], ds)

    n = lax.div(iq * bq, bk)
    lax.fori_loop(0, n, lambda j, _: block(pl.multiple_of(j * bk, bk), bk, False), None)
    for r in range(1, bk // bq):

        @pl.when(lax.rem(iq, bk // bq) >= r)
        def _():
            block(pl.multiple_of(n * bk + (r - 1) * bq, bq), bq, False)

    block(pl.multiple_of(iq * bq, bq), bq, True)
    for _, h in pieces:
        d = (dq_s[h] * scale).T.astype(bf16).astype(f32)
        dq_ref[:, heads(h)] = turn(d, cos_ref[...], -sin_ref[...]).astype(bf16)

    @pl.when(iq == steps - 3)
    def _():
        for c in parts(1):
            c.wait()
        for m in range(3):
            twos[m].wait_recv()
            three_s[m] = add(part_s[0, m, 0], part_s[0, m, 1], got_two[m, 0]).astype(bf16)

    @pl.when(iq == steps - 1)
    def _():
        for i in range(kv):
            d = (dk_s[i] * scale).astype(bf16).astype(f32)
            dkv_ref[:, heads(i)] = turn(d, cosk_ref[...], -sink_ref[...]).astype(bf16)
            dkv_ref[:, heads(kv + i)] = dv_s[i].astype(bf16)
        total = 0.0
        for m in range(3):
            threes[m].wait_recv()
            own = add(part_s[1, m, 0], part_s[1, m, 1], got_two[m, 1], got_three[m]).astype(bf16)
            if m < 2:
                sum_ref[m] = own
            else:
                last_ref[...] = own.T
            total += jnp.sum(jnp.square(own.astype(f32)))
        square_ref[...] = jnp.full(square_ref.shape, total, f32)
        for c in twos + threes:
            c.wait_send()


def attn_back(number, q, k, v, o, do, lse, cos, sin, mine, came, bq=256, bk=512):
    t, w = q.shape
    kv, h = k.shape[1] // HEAD, w // HEAD
    d, bf = mine.shape[2:]
    rows = lambda w: pl.BlockSpec((bq, w), lambda i: (i, 0))
    hbm = pl.BlockSpec(memory_space=pl.ANY)
    dma = pltpu.SemaphoreType.DMA
    return pl.pallas_call(
        functools.partial(_attn_back, kv=kv, g=h // kv, bq=bq, bk=bk, scale=HEAD**-0.5),
        grid=(t // bq,),
        in_specs=[rows(w), once(k.shape), once(v.shape), rows(w), rows(w), pl.BlockSpec((h, bq), lambda i: (0, i)), rows(HEAD), rows(HEAD),
                  once((t, HEAD)), once((t, HEAD)), hbm, hbm],
        out_specs=[rows(w), once((t, 2 * kv * HEAD)), once((2, d, bf)), once((bf, d)), once((8, 128))],
        out_shape=[jax.ShapeDtypeStruct((t, w), bf16), jax.ShapeDtypeStruct((t, 2 * kv * HEAD), bf16), jax.ShapeDtypeStruct((2, d, bf), bf16),
                   jax.ShapeDtypeStruct((bf, d), bf16), jax.ShapeDtypeStruct((8, 128), f32)],
        scratch_shapes=[pltpu.VMEM((h, HEAD, bq), f32), pltpu.VMEM((kv, t, HEAD), f32), pltpu.VMEM((kv, t, HEAD), f32),
                        pltpu.VMEM((kv, HEAD, t), bf16), pltpu.VMEM((h, bq), f32), pltpu.VMEM((2, 3, 2, d, bf), bf16),
                        pltpu.VMEM((3, 2, d, bf), bf16), pltpu.VMEM((3, 2, d, bf), bf16), pltpu.VMEM((3, d, bf), bf16), pltpu.VMEM((3, d, bf), bf16),
                        dma((2, 3, 2)), dma((3,)), dma((3,)), dma((3,)), dma((3,))],
        compiler_params=pltpu.CompilerParams(dimension_semantics=("arbitrary",), vmem_limit_bytes=VMEM, collective_id=3 + number, has_side_effects=True),
        cost_estimate=cost(8 * t * t * w, 12 * t * w),
        name=f"attn_back_{number}",
    )(q, k, v, o, do, lse, cos, sin, cos, sin, mine, came)


def _out(o_ref, wo_ref, h_ref, h1_ref, b_ref, bT_ref):
    for at in range(0, h_ref.shape[0], 256):
        here = slice(at, at + 256)
        h1 = (h_ref[here, :].astype(f32) + dot(o_ref[here, :], wo_ref[0]).astype(bf16).astype(f32)).astype(bf16)
        h1_ref[here, :] = h1
        wide, r = rms(h1)
        b = (wide * r).astype(bf16)
        b_ref[here, :] = b
        bT_ref[:, here] = b.T


def out(number, o, wo, h, rows=512):
    t, d = h.shape
    block = pl.BlockSpec((rows, d), lambda i: (i, 0))
    return pl.pallas_call(
        _out,
        grid=(t // rows,),
        in_specs=[pl.BlockSpec((rows, o.shape[1]), lambda i: (i, 0)), once((1, *wo.shape[1:]), (number, 0, 0)), block],
        out_specs=[block, block, pl.BlockSpec((d, rows), lambda i: (0, i))],
        out_shape=[jax.ShapeDtypeStruct((t, d), bf16)] * 2 + [jax.ShapeDtypeStruct((d, t), bf16)],
        compiler_params=params("arbitrary"),
        cost_estimate=cost(2 * t * d * d, 12 * t * d),
        name=f"out_{number}",
    )(o, wo, h)


def _in_back(dq_ref, dkv_ref, wq_ref, wk_ref, wv_ref, h_ref, dh1_ref, dh_ref, dhT_ref):
    n = wk_ref.shape[2]
    for at in range(0, h_ref.shape[0], 256):
        here = slice(at, at + 256)
        by_a = dot(dq_ref[here, :], wq_ref[0], 1, 1) + dot(dkv_ref[here, :n], wk_ref[0], 1, 1) + dot(dkv_ref[here, n:], wv_ref[0], 1, 1)
        dh = (dh1_ref[here, :].astype(f32) + norm_back(h_ref[here, :], by_a.astype(bf16).astype(f32))).astype(bf16)
        dh_ref[here, :] = dh
        dhT_ref[:, here] = dh.T


def in_back(number, dq, dkv, wq, wk, wv, h, dh1, rows=512):
    t, d = h.shape
    block = lambda w: pl.BlockSpec((rows, w), lambda i: (i, 0))
    return pl.pallas_call(
        _in_back,
        grid=(t // rows,),
        in_specs=[block(dq.shape[1]), block(dkv.shape[1])] + [once((1, *w.shape[1:]), (number, 0, 0)) for w in (wq, wk, wv)] + [block(d)] * 2,
        out_specs=[block(d), pl.BlockSpec((d, rows), lambda i: (0, i))],
        out_shape=[jax.ShapeDtypeStruct((t, d), bf16), jax.ShapeDtypeStruct((d, t), bf16)],
        compiler_params=params("arbitrary"),
        cost_estimate=cost(2 * t * d * (dq.shape[1] + dkv.shape[1]), 12 * t * d),
        name=f"in_back_{number}",
    )(dq, dkv, wq, wk, wv, h, dh1)


def gated(g):
    s = 1 / (1 + jnp.exp(-g))
    return s, g * s


def _mlp(b_ref, h1_ref, wg_ref, wu_ref, wd_ref, h2_ref, act_ref, by_g_ref, by_u_ref, acc_s, *, bm):
    j = pl.program_id(0)
    t = b_ref.shape[0]

    @pl.when(j == 0)
    def _():
        acc_s[...] = jnp.zeros_like(acc_s)

    rows = [pl.ds(i * bm, bm) for i in range(t // bm)]
    for i, r in enumerate(rows):
        g, u = dot(b_ref[r, :], wg_ref[0]), dot(b_ref[r, :], wu_ref[0])
        s, silu = gated(g)
        act_ref[0, r, :] = (silu * u).astype(bf16)
        by_g_ref[0, r, :] = u * (s * (1 + g * (1 - s)))
        by_u_ref[0, r, :] = silu
    for r in rows:
        acc_s[r, :] += dot(act_ref[0, r, :], wd_ref[0])

    @pl.when(j == pl.num_programs(0) - 1)
    def _():
        h2_ref[...] = (h1_ref[...].astype(f32) + acc_s[...].astype(bf16).astype(f32)).astype(bf16)


def mlp(number, b, h1, wg, wu, wd, bf=256, bm=512):
    t, d = b.shape
    n = wg.shape[2] // bf
    col = pl.BlockSpec((1, d, bf), lambda j: (number, 0, j))
    kept = pl.BlockSpec((1, t, bf), lambda j: (j, 0, 0))
    return pl.pallas_call(
        functools.partial(_mlp, bm=bm),
        grid=(n,),
        in_specs=[once((t, d)), once((t, d)), col, col, pl.BlockSpec((1, bf, d), lambda j: (number, j, 0))],
        out_specs=[once((t, d)), kept, kept, kept],
        out_shape=[jax.ShapeDtypeStruct((t, d), bf16), jax.ShapeDtypeStruct((n, t, bf), bf16)] + [jax.ShapeDtypeStruct((n, t, bf), f32)] * 2,
        scratch_shapes=[pltpu.VMEM((t, d), f32)],
        compiler_params=params("arbitrary"),
        cost_estimate=cost(6 * t * d * n * bf, 8 * t * n * bf),
        name=f"mlp_{number}",
    )(b, h1, wg, wu, wd)


def block_of(i, me):
    slot = lax.rem(3 * (7 - lax.rem(i, 8)), 8) * 2 + 1 - lax.div(i, 8)
    return sum(lax.rem(bit(slot, k) + bit(me, k), 2) * 2**k for k in range(4))


AXES = ((4, 3), (2, 2), (1, 1))


def chip_slot(k):
    return 3 * (7 - k) % 8 if isinstance(k, int) else lax.rem(3 * (7 - k), 8)


def _gated_back(*refs, stored, bm, deep):
    it = iter(refs)
    b_hbm = None if stored else next(it)
    bT_hbm, dh_hbm, dhT_hbm, h1_hbm, wo_ref, wg_ref, wu_ref, wd_ref = (next(it) for _ in range(8))
    act_ref, by_g_ref, by_u_ref = (next(it) for _ in range(3)) if stored else (None, None, None)
    dh1_hbm, do_hbm, mine, came, core_in = (next(it) for _ in range(5))
    b_s, act_s = (None, None) if stored else (next(it), next(it))
    (acc_s, bT_s, dh_s, dhT_s, h1_s, dgu_s, wgu_s, term_s, recv_s, load_sem, back_sem, core_send, core_recv, out_send, out_recv,
     keep_sem, recv_sem) = (next(it) for _ in range(17))
    i, me = pl.program_id(0), lax.axis_index("dp")
    t, bf = dgu_s.shape[0], dgu_s.shape[1] // 2

    def to_core(k):
        return pltpu.make_async_remote_copy(term_s.at[lax.rem(k, deep)], core_in.at[k], core_send.at[k], core_recv.at[k],
                                            device_id={"dp": flip(me, 0)}, device_id_type=pl.DeviceIdType.MESH)

    def to_chip(m, k):
        slot, (half, axis) = chip_slot(k), AXES[m]
        return pltpu.make_async_remote_copy(term_s.at[lax.rem(k + 8, deep), m], came.at[m, slot - half], out_send.at[m, k], out_recv.at[m, slot - half],
                                            device_id={"dp": flip(me, axis)}, device_id_type=pl.DeviceIdType.MESH)

    def keep(m, k):
        return pltpu.make_async_copy(term_s.at[lax.rem(k + 8, deep), m], mine.at[m, chip_slot(k)], keep_sem.at[m, k])

    def move(k, act):
        @pl.when(k < 8)
        def _():
            act(to_core(k))

        @pl.when(k >= 8)
        def _():
            for m in range(3):
                out = lax.rem(lax.div(chip_slot(k - 8), AXES[m][0]), 2) == 1

                @pl.when(out)
                def _():
                    act(to_chip(m, k - 8))

                @pl.when(jnp.logical_not(out))
                def _():
                    act(keep(m, k - 8))

    def start(c):
        c.start()

    def finish(c):
        (c.wait_send if hasattr(c, "wait_send") and c.is_remote else c.wait)()

    loads = [pltpu.make_async_copy(src, dst, load_sem.at[n]) for n, (src, dst) in enumerate(
        [(dh_hbm, dh_s)] + ([] if stored else [(b_hbm, b_s)]) + [(bT_hbm, bT_s), (dhT_hbm, dhT_s)])]
    first = 1 if stored else 2

    @pl.when(i == 0)
    def _():
        for c in loads:
            c.start()
        acc_s[...] = jnp.zeros_like(acc_s)
        recv_s[...] = jnp.zeros_like(recv_s)
        barrier = pltpu.get_barrier_semaphore()
        for axis in range(4):
            pl.semaphore_signal(barrier, inc=1, device_id={"dp": flip(me, axis)}, device_id_type=pl.DeviceIdType.MESH)
        pl.semaphore_wait(barrier, 4)
        for c in loads[:first]:
            c.wait()

    @pl.when(i >= 1)
    def _():
        move(i - 1, start)

    landed = pltpu.make_async_copy(core_in.at[lax.rem(i, 8)], recv_s, recv_sem.at[0])

    @pl.when(i >= 8)
    def _():
        to_core(i - 8).wait_recv()
        landed.start()

    wgu_s[:, :bf] = wg_ref[0]
    wgu_s[:, bf:] = wu_ref[0]
    rows = [pl.ds(r * bm, bm) for r in range(t // bm)]
    for r in rows:
        da = dot(dh_s[r, :], wd_ref[0], 1, 1).astype(bf16).astype(f32)
        if stored:
            by_g, by_u = by_g_ref[0, r, :], by_u_ref[0, r, :]
        else:
            gu = dot(b_s[r, :], wgu_s[...])
            g, u = gu[:, :bf], gu[:, bf:]
            s, by_u = gated(g)
            by_g = u * (s * (1 + g * (1 - s)))
            act_s[r, :] = (by_u * u).astype(bf16)
        dgu_s[r, bf:] = (da * by_u).astype(bf16)
        dgu_s[r, :bf] = (da * by_g).astype(bf16)
    for r in rows:
        acc_s[r, :] += dot(dgu_s[r, :], wgu_s[...], 1, 1)

    @pl.when(i == 0)
    def _():
        for c in loads[first:]:
            c.wait()

    @pl.when(i >= deep)
    def _():
        move(i - deep, finish)

    @pl.when(i >= 8)
    def _():
        landed.wait()

    place = lax.rem(i, deep)
    dgu = dot(bT_s[...], dgu_s[...])
    for m, term in enumerate((dgu[:, :bf], dgu[:, bf:], dot(dhT_s[...], act_ref[0] if stored else act_s[...]))):
        term_s[place, m] = (term + recv_s[m].astype(f32)).astype(bf16)

    @pl.when(i == 15)
    def _():
        for m in range(3):
            keep(m, 7).start()
        chunks = [pl.ds(n * 256, 256) for n in range(t // 256)]
        loaded = [pltpu.make_async_copy(h1_hbm.at[r], h1_s.at[n % 4], back_sem.at[0, n]) for n, r in enumerate(chunks)]
        gone = [pltpu.make_async_copy(h1_s.at[n % 4], dh1_hbm.at[r], back_sem.at[1, n]) for n, r in enumerate(chunks)]
        back = [pltpu.make_async_copy(dh_s.at[r], do_hbm.at[r], back_sem.at[2, n]) for n, r in enumerate(chunks)]
        for c in loaded[:4]:
            c.start()
        for n, r in enumerate(chunks):
            by_b = acc_s[r, :].astype(bf16).astype(f32)
            loaded[n].wait()
            dh1 = (dh_s[r, :].astype(f32) + norm_back(h1_s[n % 4], by_b)).astype(bf16)
            h1_s[n % 4] = dh1
            gone[n].start()
            dh_s[r, :] = dot(dh1, wo_ref[0], 1, 1).astype(bf16)
            back[n].start()
            if 1 <= n < len(chunks) - 3:
                gone[n - 1].wait()
                loaded[n + 3].start()
        for m in range(3):
            for k in range(8):
                out = chip_slot(k) // AXES[m][0] % 2 == 1
                if out:
                    to_chip(m, k).wait_recv()
                if k > 7 - deep:
                    to_chip(m, k).wait_send() if out else keep(m, k).wait()
        for c in gone[len(chunks) - 4 :] + back:
            c.wait()


def gated_back(number, bT, dh, dhT, h1, wg, wu, wd, wo, b=None, kept=None, bf=256, bm=512, deep=3):
    d, t = bT.shape
    stored = kept is not None
    col = pl.BlockSpec((1, d, bf), lambda i: (number, 0, block_of(i, lax.axis_index("dp"))))
    held = pl.BlockSpec((1, t, bf), lambda i: (block_of(i, lax.axis_index("dp")), 0, 0))
    hbm = pl.BlockSpec(memory_space=pl.ANY)
    given = ([] if stored else [b]) + [bT, dh, dhT, h1, wo, wg, wu, wd] + (list(kept) if stored else [])
    specs = [hbm] * (4 if stored else 5) + [once((1, *wo.shape[1:]), (number, 0, 0)), col, col]
    specs += [pl.BlockSpec((1, bf, d), lambda i: (number, block_of(i, lax.axis_index("dp")), 0))] + ([held] * 3 if stored else [])
    dma = pltpu.SemaphoreType.DMA
    got = pl.pallas_call(
        functools.partial(_gated_back, stored=stored, bm=bm, deep=deep),
        grid=(16,),
        in_specs=specs,
        out_specs=[hbm] * 5,
        out_shape=[jax.ShapeDtypeStruct((t, d), bf16), jax.ShapeDtypeStruct((t, wo.shape[1]), bf16)]
        + [jax.ShapeDtypeStruct((3, 8, d, bf), bf16)] * 2 + [jax.ShapeDtypeStruct((8, 3, d, bf), bf16)],
        scratch_shapes=([] if stored else [pltpu.VMEM((t, d), bf16), pltpu.VMEM((t, bf), bf16)])
        + [pltpu.VMEM((t, d), f32), pltpu.VMEM((d, t), bf16), pltpu.VMEM((t, d), bf16), pltpu.VMEM((d, t), bf16), pltpu.VMEM((4, 256, d), bf16),
           pltpu.VMEM((t, 2 * bf), bf16), pltpu.VMEM((d, 2 * bf), bf16), pltpu.VMEM((deep, 3, d, bf), bf16),
           pltpu.VMEM((3, d, bf), bf16), dma((4,)), dma((3, t // 256)), dma((8,)), dma((8,)), dma((3, 8)), dma((3, 8)), dma((3, 8)), dma((1,))],
        compiler_params=pltpu.CompilerParams(dimension_semantics=("arbitrary",), vmem_limit_bytes=VMEM, collective_id=1 + number, has_side_effects=True),
        cost_estimate=cost(2 * t * d * bf * 16 * (6 if stored else 8), 8 * t * bf * 16),
        name=f"gated_back_{number}",
    )(*given)
    return got[:4]


def _attn_sums(dq_ref, dk_ref, dv_ref, dh1_ref, square_ref, aT_hbm, oT_hbm, own_ref, factor_ref,
               aT_s, oT_s, right_s, term_s, from_core, sum_s, one_s, got_one, two_s, got_two, three_s, got_three, sq_s, got_sq,
               load_sem, core_sem, send_sem, recv_sem, sq_send, sq_recv, *, count):
    i, me = pl.program_id(0), lax.axis_index("dp")
    chip = lax.div(me, 2)
    to = lambda axis: dict(device_id={"dp": flip(me, axis)}, device_id_type=pl.DeviceIdType.MESH)
    q, n, w = dq_ref.shape[1], dk_ref.shape[1], from_core.shape[1]
    d, third, high = from_core.shape[0], w // 3, from_core.shape[0] // 8
    loads = [pltpu.make_async_copy(aT_hbm, aT_s, load_sem.at[0]), pltpu.make_async_copy(oT_hbm, oT_s, load_sem.at[1])]
    to_core = pltpu.make_async_remote_copy(term_s, from_core, core_sem.at[0], core_sem.at[1], **to(0))

    @pl.when(i == 0)
    def _():
        for c in loads:
            c.start()
        barrier = pltpu.get_barrier_semaphore()
        pl.semaphore_signal(barrier, inc=1, **to(0))
        for n in range(1, 8):
            pl.semaphore_signal(barrier, inc=1, device_id={"dp": flips(me, 2 * n)}, device_id_type=pl.DeviceIdType.MESH)
        pl.semaphore_wait(barrier, 8)

    @pl.when(i == 1)
    def _():
        to_core.start()

    right_s[:, :q] = dq_ref[...]
    right_s[:, q : q + n] = dk_ref[...]
    right_s[:, q + n :] = dv_ref[...]

    @pl.when(i == 0)
    def _():
        for c in loads:
            c.wait()

    sum_s[:, : q + 2 * n] = dot(aT_s[...], right_s[...])
    sum_s[:, q + 2 * n :] = dot(oT_s[...], dh1_ref[...])

    @pl.when(i == 0)
    def _():
        term_s[...] = sum_s[...].astype(bf16)

    @pl.when(i == 1)
    def _():
        to_core.wait()

        def mine(m, slot):
            rows = pl.ds(pl.multiple_of(flips(chip, slot) * high, high), high)
            cols = slice(m * third, (m + 1) * third)
            return add(sum_s[rows, cols], from_core[rows, cols])

        def exchange(phase, src, dst):
            cs = [pltpu.make_async_remote_copy(src.at[m], dst.at[m], send_sem.at[phase, m], recv_sem.at[phase, m], **to(PLACE[TURN[m][phase]])) for m in range(3)]
            for c in cs:
                c.start()
            return cs

        for m, (a, b, c) in enumerate(TURN):
            for at, rest in enumerate((b | c, b, c, 0)):
                one_s[m, at] = mine(m, a | rest).astype(bf16)
        ones = exchange(0, one_s, got_one)
        for m, (a, b, c) in enumerate(TURN):
            ones[m].wait_recv()
            for at, rest in enumerate((b | c, b)):
                two_s[m, at] = add(mine(m, rest), got_one[m, at]).astype(bf16)
        twos = exchange(1, two_s, got_two)
        for m, (a, b, c) in enumerate(TURN):
            twos[m].wait_recv()
            three_s[m] = add(mine(m, c), got_one[m, 2], got_two[m, 0]).astype(bf16)
        threes = exchange(2, three_s, got_three)
        total = jnp.zeros((8, 128), f32)
        for n in range(square_ref.shape[0]):
            total += square_ref[n]
        own_square = 0.0
        for m in range(3):
            threes[m].wait_recv()
            own = add(mine(m, 0), got_one[m, 3], got_two[m, 1], got_three[m]).astype(bf16)
            own_ref[:, m * third : (m + 1) * third] = own
            own_square += jnp.sum(jnp.square(own.astype(f32)))
        total += own_square
        sq_s[0] = total
        c = pltpu.make_async_remote_copy(sq_s.at[0], got_sq.at[0], sq_send.at[0], sq_recv.at[0], **to(0))
        c.start()
        c.wait()
        sq_s[1] = total + got_sq[0]
        cs = [pltpu.make_async_remote_copy(sq_s.at[1], got_sq.at[n], sq_send.at[n], sq_recv.at[n], device_id={"dp": flips(me, 2 * n)},
                                           device_id_type=pl.DeviceIdType.MESH) for n in range(1, 8)]
        for c in cs:
            c.start()
        for c in cs:
            c.wait()
        got_sq[0] = sq_s[1]
        total = got_sq[chip]
        for n in range(1, 8):
            total = total + got_sq[flips(chip, n)]
        factor_ref[...] = jnp.minimum(1.0, 0.5 * lax.rsqrt(total / count + 1e-30))
        for c in ones + twos + threes:
            c.wait_send()


def attn_sums(aT, dq, dkv, oT, dh1, squares, count):
    d, t = aT.shape
    n = dkv.shape[1] // 4
    q, o = dq.shape[1] // 2, dh1.shape[1] // 2
    w = q + 2 * n + o
    third, high = w // 3, d // 8
    half = lambda i: lax.rem(lax.rem(lax.axis_index("dp"), 2) + 1 + i, 2)
    hbm = pl.BlockSpec(memory_space=pl.ANY)
    dma = pltpu.SemaphoreType.DMA
    return pl.pallas_call(
        functools.partial(_attn_sums, count=count),
        grid=(2,),
        in_specs=[pl.BlockSpec((t, q), lambda i: (0, half(i))),
                  pl.BlockSpec((t, n), lambda i: (0, half(i))),
                  pl.BlockSpec((t, n), lambda i: (0, 2 + half(i))),
                  pl.BlockSpec((t, o), lambda i: (0, half(i))),
                  once(squares.shape), hbm, hbm],
        out_specs=[once((high, w)), once((8, 128))],
        out_shape=[jax.ShapeDtypeStruct((high, w), bf16), jax.ShapeDtypeStruct((8, 128), f32)],
        scratch_shapes=[pltpu.VMEM((d, t), bf16), pltpu.VMEM((d, t), bf16), pltpu.VMEM((t, q + 2 * n), bf16), pltpu.VMEM((d, w), bf16),
                        pltpu.VMEM((d, w), bf16), pltpu.VMEM((d, w), f32)]
        + [pltpu.VMEM((3, 4, high, third), bf16)] * 2 + [pltpu.VMEM((3, 2, high, third), bf16)] * 2 + [pltpu.VMEM((3, high, third), bf16)] * 2
        + [pltpu.VMEM((2, 8, 128), f32), pltpu.VMEM((8, 8, 128), f32)] + [dma((2,)), dma((2,)), dma((3, 3)), dma((3, 3)), dma((8,)), dma((8,))],
        compiler_params=pltpu.CompilerParams(dimension_semantics=("arbitrary",), vmem_limit_bytes=VMEM, collective_id=5, has_side_effects=True),
        cost_estimate=cost(4 * t * d * w, 16 * t * d),
        name="attn_sums",
    )(dq, dkv, dkv, dh1, squares, aT, oT)


def _adamw(factor_ref, *refs, widths, form, old):
    k = len(widths)
    gs = k if form != "cores" else 1
    ins, gs, outs = refs[: 3 * k], refs[3 * k : 3 * k + gs], refs[3 * k + gs + old * 3 * k :]
    factor = factor_ref[:1, :1]

    def one(a, cols, g):
        w_ref, m_ref, v_ref = ins[3 * a : 3 * a + 3]
        nw_ref, nm_ref, nv_ref = outs[3 * a : 3 * a + 3]
        g = g.astype(f32) * factor
        m = 0.9 * m_ref[0, :, cols] + 0.1 * g
        v = 0.95 * v_ref[0, :, cols] + 0.05 * g * g
        w = w_ref[0, :, cols].astype(f32)
        nm_ref[0, :, cols] = m
        nv_ref[0, :, cols] = v
        nw_ref[0, :, cols] = (w - 0.02 * (m * lax.rsqrt(v + 1e-8) + 0.1 * w)).astype(bf16)

    for a, width in enumerate(widths):
        if form == "cores":
            at = sum(widths[:a]) // 2
            for c in range(2):
                one(a, slice(c * width // 2, (c + 1) * width // 2), gs[0][0, c, :, at : at + width // 2])
        elif len(gs[a].shape) == 3:
            n, wide = gs[a].shape[0], gs[a].shape[2]
            for c in range(n):
                one(a, slice(c * wide, (c + 1) * wide), gs[a][c])
        else:
            one(a, slice(None), gs[a][...])


def adamw(number, factor, arrays, gs, before=None, form="", rows=32):
    height = arrays[0][0].shape[1]
    widths = [a[0].shape[2] for a in arrays]
    given, specs, out_specs, out_shape = [factor], [once(factor.shape)], [], []
    for (w, m, v), width in zip(arrays, widths):
        block = pl.BlockSpec((1, rows, width), lambda i: (number, i, 0))
        given += [w, m, v]
        specs += [block] * 3
        out_specs += [block] * 3
        out_shape += [jax.ShapeDtypeStruct(w.shape, bf16), jax.ShapeDtypeStruct(m.shape, f32), jax.ShapeDtypeStruct(v.shape, f32)]
    for g in gs:
        given += [g]
        if form == "cores":
            per = g.shape[2] // rows
            specs += [pl.BlockSpec((1, 2, rows, g.shape[3]), lambda i: (lax.div(i, per), 0, lax.rem(i, per), 0))]
        elif g.ndim == 3:
            specs += [pl.BlockSpec((g.shape[0], rows, g.shape[2]), lambda i: (0, i, 0))]
        else:
            specs += [pl.BlockSpec((rows, g.shape[1]), lambda i: (i, 0))]
    alias = {}
    if before is not None:
        flat = [x for one in before for x in one]
        alias = {len(given) + i: i for i in range(len(flat))}
        given += flat
        specs += [pl.BlockSpec(memory_space=pl.ANY)] * len(flat)
    got = pl.pallas_call(
        functools.partial(_adamw, widths=widths, form=form, old=int(before is not None)),
        grid=(height // rows,),
        in_specs=specs,
        out_specs=out_specs,
        out_shape=out_shape,
        input_output_aliases=alias,
        compiler_params=params("arbitrary"),
        cost_estimate=cost(20 * height * sum(widths), 22 * height * sum(widths)),
        name=f"adamw_{number}_{len(arrays)}",
    )(*given)
    return [tuple(got[3 * a : 3 * a + 3]) for a in range(len(arrays))]


def solution(mesh):
    def step(x, dy, *arrays):
        weights, first, second = (dict(zip(NAMES, arrays[i : i + 7], strict=True)) for i in (0, 7, 14))
        wq, wk, wv, wo, wg, wu, wd = (weights[name] for name in NAMES)
        x, dy = x[0], dy[0]
        t, d = x.shape
        me = lax.axis_index("dp").astype(jnp.int32)
        half = HEAD // 2
        angle = jnp.arange(t, dtype=f32)[:, None] * THETA ** (-jnp.arange(half, dtype=f32) / half)
        cos = jnp.concatenate([jnp.cos(angle)] * 2, 1)
        sin = jnp.concatenate([-jnp.sin(angle), jnp.sin(angle)], 1)

        q0, k0, v0, aT0, dyT = qkv(0, x, wq, wk, wv, cos, sin, also=dy)
        o0, oT0, lse0 = attn(0, q0, k0, v0)
        h01, b0, bT0 = out(0, o0, wo, x)
        h1, *kept0 = mlp(0, b0, h01, wg, wu, wd)
        q1, k1, v1, aT1 = qkv(1, h1, wq, wk, wv, cos, sin)
        o1, oT1, lse1 = attn(1, q1, k1, v1)
        h11, b1, bT1 = out(1, o1, wo, h1)

        def gather(sums, last):
            return [lax.all_gather(s, "dp") for s in (sums[0], sums[1])] + [lax.all_gather(last, "dp", tiled=True)]

        def matmul(a, b):
            return jnp.dot(a, b, preferred_element_type=f32).astype(bf16)

        after = lambda *xs: lax.optimization_barrier(xs)
        dh11, do1, mine, came = gated_back(1, bT1, dy, dyT, h11, wg, wu, wd, wo, b=b1)
        dq1, dkv1, sums1, last1, square1 = attn_back(1, q1, k1, v1, o1, do1, lse1, cos, sin, mine, came)
        gathered1 = gather(sums1, last1)
        dh, dhT = in_back(1, dq1, dkv1, wq, wk, wv, h1, dh11)
        rest1 = lax.psum((matmul(aT1, dq1), matmul(aT1, dkv1), matmul(oT1, dh11)), "dp")
        dh01, do0, mine, came = gated_back(0, bT0, dh, dhT, h01, wg, wu, wd, wo, kept=kept0)
        do0, gathered1[0] = after(do0, gathered1[0])
        dq0, dkv0, sums0, last0, square0 = attn_back(0, q0, k0, v0, o0, do0, lse0, cos, sin, mine, came)
        dq0, gathered1[1] = after(dq0, gathered1[1])
        gathered0 = gather(sums0, last0)
        own = d // DEVICES
        square_rest = sum(jnp.sum(jnp.square(lax.dynamic_slice_in_dim(g, own * me, own).astype(f32))) for g in rest1)
        squares = jnp.stack([square1, square0, jnp.full((8, 128), square_rest)])
        part0, factor = attn_sums(aT0, dq0, dkv0, oT0, dh01, squares, sum(w.size for w in weights.values()))
        rest0 = lax.all_gather(part0, "dp").reshape(DEVICES // 2, 2, *part0.shape)
        n = wk.shape[2]
        rest1 = [rest1[0], rest1[1][:, :n], rest1[1][:, n:], rest1[2]]

        of = lambda names: [(weights[name], first[name], second[name]) for name in names]
        new_attn = adamw(1, factor, of(NAMES[:4]), rest1, rows=128)
        new_up = adamw(1, factor, of(NAMES[4:6]), gathered1[:2], rows=64)
        new_down = adamw(1, factor, of(NAMES[6:]), gathered1[2:], rows=256)
        new_up = adamw(0, factor, of(NAMES[4:6]), gathered0[:2], before=new_up, rows=64)
        new_down = adamw(0, factor, of(NAMES[6:]), gathered0[2:], before=new_down, rows=256)
        new_attn = adamw(0, factor, of(NAMES[:4]), [rest0], before=new_attn, form="cores", rows=80)
        new = new_attn + new_up + new_down
        return tuple(n[which] for which in range(3) for n in new)

    states, all_of = P(("rep", "dp"), None, None), P(None, None, None)
    return jax.shard_map(
        step,
        mesh=mesh,
        in_specs=(states, states) + (all_of,) * 21,
        out_specs=(P("rep", None, None),) * 21,
        check_vma=False,
    )
```

```python
import functools

import jax
import jax.numpy as jnp
from jax import lax
from jax.experimental import pallas as pl
from jax.experimental.pallas import tpu as pltpu
from jax.sharding import PartitionSpec as P

bf16, f32 = jnp.bfloat16, jnp.float32
HEAD = 128
THETA = 10000
NAMES = ("wq", "wk", "wv", "wo", "w_gate", "w_up", "w_down")
NEG = -1e30
HIDDEN = 2 * NEG
LOG2E = 1.4426950408889634
VMEM = 63 * 2**20
DEVICES = 16
PLACE = {4: 3, 2: 2, 1: 1}
TURN = ((4, 2, 1), (2, 1, 4), (1, 4, 2))


def dot(a, b, ca=1, cb=0):
    return lax.dot_general(a, b, (((ca,), (cb,)), ((), ())), preferred_element_type=f32)


def once(shape, index=None):
    index = index or (0,) * len(shape)
    return pl.BlockSpec(shape, lambda *_: index, pipeline_mode=pl.Buffered(1))


def params(*semantics):
    return pltpu.CompilerParams(dimension_semantics=semantics, vmem_limit_bytes=VMEM)


def cost(flops, moved):
    return pl.CostEstimate(flops=flops, transcendentals=0, bytes_accessed=moved)


def rms(h):
    wide = h.astype(f32)
    return wide, lax.rsqrt(jnp.mean(wide * wide, -1, keepdims=True) + 1e-6)


def norm_back(h, by_out):
    wide, r = rms(h)
    return r * by_out - wide * (r * r * r * jnp.mean(by_out * wide, -1, keepdims=True))


def turn(t, cos, sin):
    return t * cos + pltpu.roll(t, HEAD // 2, 1) * sin


def heads(n):
    return slice(n * HEAD, (n + 1) * HEAD)


def bit(v, k):
    return lax.rem(lax.div(v, 2**k), 2)


def flip(v, k):
    return v + 2**k * (1 - 2 * bit(v, k))


def flips(v, mask):
    for k in range(4):
        if mask // 2**k % 2:
            v = flip(v, k)
    return v


def add(*terms):
    return functools.reduce(lambda a, b: a + b, [t.astype(f32) for t in terms])


def _qkv(*refs, extra):
    h_ref, wq_ref, wk_ref, wv_ref, cos_ref, sin_ref = refs[:6]
    q_ref, k_ref, v_ref, aT_ref = refs[6 + extra : 10 + extra]
    for at in range(0, h_ref.shape[0], 256):
        here = slice(at, at + 256)
        wide, r = rms(h_ref[here, :])
        a = (wide * r).astype(bf16)
        aT_ref[:, here] = a.T
        cos, sin = cos_ref[here, :], sin_ref[here, :]
        for w_ref, out_ref in ((wq_ref, q_ref), (wk_ref, k_ref)):
            t = dot(a, w_ref[0]).astype(bf16).astype(f32)
            for n in range(t.shape[1] // HEAD):
                out_ref[here, heads(n)] = turn(t[:, heads(n)], cos, sin).astype(bf16)
        v_ref[here, :] = dot(a, wv_ref[0]).astype(bf16)
        if extra:
            refs[-1][:, here] = refs[6][here, :].T


def qkv(number, h, wq, wk, wv, cos, sin, also=None, rows=512):
    t, d = h.shape
    block = lambda w: pl.BlockSpec((rows, w), lambda i: (i, 0))
    across = pl.BlockSpec((d, rows), lambda i: (0, i))
    extra = also is not None
    return pl.pallas_call(
        functools.partial(_qkv, extra=int(extra)),
        grid=(t // rows,),
        in_specs=[block(d)] + [once((1, *w.shape[1:]), (number, 0, 0)) for w in (wq, wk, wv)] + [block(HEAD)] * 2 + [block(d)] * extra,
        out_specs=[block(w.shape[2]) for w in (wq, wk, wv)] + [across] * (1 + extra),
        out_shape=[jax.ShapeDtypeStruct((t, w.shape[2]), bf16) for w in (wq, wk, wv)] + [jax.ShapeDtypeStruct((d, t), bf16)] * (1 + extra),
        compiler_params=params("arbitrary"),
        cost_estimate=cost(2 * t * d * sum(w.shape[2] for w in (wq, wk, wv)), 8 * t * d),
        name=f"qkv_{number}",
    )(h, wq, wk, wv, cos, sin, *([also] if extra else []))


def _attn(q_ref, k_ref, v_ref, o_ref, oT_ref, lse_ref, top_s, mix_s, vT_s, *, kv, g, bq, bk, scale):
    iq = pl.program_id(0)
    t = k_ref.shape[0]
    e = scale * LOG2E

    @pl.when(iq == 0)
    def _():
        for i in range(kv):
            vT_s[i, :HEAD, :] = v_ref[:, heads(i)].T
            vT_s[i, HEAD:, :] = jnp.ones((16, t), bf16)

    pieces = [(i, i * g + n) for i in range(kv) for n in range(g)]
    top_s[...] = jnp.full_like(top_s, NEG)
    mix_s[...] = jnp.zeros_like(mix_s)

    def block(start, size, masked):
        here = pl.ds(start, size)
        scores = [dot(k_ref[here, heads(i)], q_ref[:, heads(h)], 1, 1) for i, h in pieces]
        if masked:
            ok = lax.broadcasted_iota(jnp.int32, (size, bq), 1) >= lax.broadcasted_iota(jnp.int32, (size, bq), 0)
        weights, keeps = [], []
        for (_, h), s in zip(pieces, scores):
            if masked:
                s = jnp.where(ok, s, HIDDEN)
            old = top_s[h : h + 1, :]
            top = jnp.maximum(old, s.max(axis=0, keepdims=True))
            top_s[h : h + 1, :] = top
            weights.append(jnp.exp2((s - top) * e).astype(bf16))
            keeps.append(jnp.exp2((old - top) * e))
        for (i, h), p, keep in zip(pieces, weights, keeps):
            mix_s[h] = mix_s[h] * keep + dot(vT_s[i, :, here], p)

    n = lax.div(iq * bq, bk)
    lax.fori_loop(0, n, lambda j, _: block(pl.multiple_of(j * bk, bk), bk, False), None)
    for r in range(1, bk // bq):

        @pl.when(lax.rem(iq, bk // bq) >= r)
        def _():
            block(pl.multiple_of(n * bk + (r - 1) * bq, bq), bq, False)

    block(pl.multiple_of(iq * bq, bq), bq, True)
    for _, h in pieces:
        total = mix_s[h, HEAD : HEAD + 1, :]
        out = mix_s[h, :HEAD, :] * (1 / total)
        oT_ref[heads(h), :] = out.astype(bf16)
        o_ref[:, heads(h)] = out.T.astype(bf16)
        lse_ref[h : h + 1, :] = top_s[h : h + 1, :] * scale + jnp.log(total)


def attn(number, q, k, v, bq=256, bk=512):
    t, w = q.shape
    kv, h = k.shape[1] // HEAD, w // HEAD
    return pl.pallas_call(
        functools.partial(_attn, kv=kv, g=h // kv, bq=bq, bk=bk, scale=HEAD**-0.5),
        grid=(t // bq,),
        in_specs=[pl.BlockSpec((bq, w), lambda i: (i, 0)), once(k.shape), once(v.shape)],
        out_specs=[pl.BlockSpec((bq, w), lambda i: (i, 0)), pl.BlockSpec((w, bq), lambda i: (0, i)), pl.BlockSpec((h, bq), lambda i: (0, i))],
        out_shape=[jax.ShapeDtypeStruct((t, w), bf16), jax.ShapeDtypeStruct((w, t), bf16), jax.ShapeDtypeStruct((h, t), f32)],
        scratch_shapes=[pltpu.VMEM((h, bq), f32), pltpu.VMEM((h, HEAD + 16, bq), f32), pltpu.VMEM((kv, HEAD + 16, t), bf16)],
        compiler_params=params("arbitrary"),
        cost_estimate=cost(4 * t * t * w, 8 * t * w),
        name=f"attn_{number}",
    )(q, k, v)


def _out(o_ref, wo_ref, h_ref, h1_ref, b_ref, bT_ref):
    for at in range(0, h_ref.shape[0], 256):
        here = slice(at, at + 256)
        h1 = (h_ref[here, :].astype(f32) + dot(o_ref[here, :], wo_ref[0]).astype(bf16).astype(f32)).astype(bf16)
        h1_ref[here, :] = h1
        wide, r = rms(h1)
        b = (wide * r).astype(bf16)
        b_ref[here, :] = b
        bT_ref[:, here] = b.T


def out(number, o, wo, h, rows=512):
    t, d = h.shape
    block = pl.BlockSpec((rows, d), lambda i: (i, 0))
    return pl.pallas_call(
        _out,
        grid=(t // rows,),
        in_specs=[pl.BlockSpec((rows, o.shape[1]), lambda i: (i, 0)), once((1, *wo.shape[1:]), (number, 0, 0)), block],
        out_specs=[block, block, pl.BlockSpec((d, rows), lambda i: (0, i))],
        out_shape=[jax.ShapeDtypeStruct((t, d), bf16)] * 2 + [jax.ShapeDtypeStruct((d, t), bf16)],
        compiler_params=params("arbitrary"),
        cost_estimate=cost(2 * t * d * d, 12 * t * d),
        name=f"out_{number}",
    )(o, wo, h)


def _attn_back(*refs, kv, g, bq, bk, scale, deeper):
    it = iter(refs)
    q_ref, k_ref, v_ref, oT_ref, do_ref, lse_ref, cos_ref, sin_ref = (next(it) for _ in range(8))
    wq_ref, wk_ref, wv_ref, h_ref, dh1_ref = (next(it) for _ in range(5)) if deeper else (None,) * 5
    mine, came, dq_ref, dkv_ref, gate_ref, up_ref, down_ref, square_ref = (next(it) for _ in range(8))
    dh_ref, dhT_ref = (next(it), next(it)) if deeper else (None, None)
    (dq_s, dk_s, dv_s, kT_s, d_s, part_s, two_s, got_two, three_s, got_three, part_sem, two_send, two_recv, three_send,
     three_recv) = it
    step, steps = pl.program_id(0), pl.num_programs(0)
    iq = steps - 1 - step
    e = scale * LOG2E
    me = lax.axis_index("dp")

    def parts(which):
        copies = []
        for m, (_, two, three) in enumerate(TURN):
            for n, slot in enumerate(((two | three, two), (three, 0))[which]):
                copies += [pltpu.make_async_copy(ref.at[m, slot], part_s.at[n, m, h], part_sem.at[n, m, h]) for h, ref in enumerate((mine, came))]
        return copies

    def across(src, dst, send, recv, turn):
        return [pltpu.make_async_remote_copy(src.at[m], dst.at[m], send.at[m], recv.at[m], device_id={"dp": flip(me, PLACE[TURN[m][turn]])},
                                             device_id_type=pl.DeviceIdType.MESH) for m in range(3)]

    twos = across(two_s, got_two, two_send, two_recv, 1)
    threes = across(three_s, got_three, three_send, three_recv, 2)

    @pl.when(step == 0)
    def _():
        for c in parts(0):
            c.start()
        dk_s[...] = jnp.zeros_like(dk_s)
        dv_s[...] = jnp.zeros_like(dv_s)
        for i in range(kv):
            kT_s[i] = k_ref[:, heads(i)].T
        barrier = pltpu.get_barrier_semaphore()
        for axis in range(1, 4):
            pl.semaphore_signal(barrier, inc=1, device_id={"dp": flip(me, axis)}, device_id_type=pl.DeviceIdType.MESH)
        pl.semaphore_wait(barrier, 3)

    @pl.when(step == 1)
    def _():
        for c in parts(1):
            c.start()
        for c in twos:
            c.start()

    @pl.when(step == steps // 2)
    def _():
        for c in threes:
            c.start()

    dq_s[...] = jnp.zeros_like(dq_s)
    pieces = [(i, i * g + n) for i in range(kv) for n in range(g)]
    for _, h in pieces:
        d_s[h : h + 1, :] = (do_ref[:, heads(h)].T.astype(f32) * oT_ref[heads(h), :].astype(f32)).sum(axis=0, keepdims=True)

    def block(start, size, masked):
        here = pl.ds(start, size)
        if masked:
            ok = lax.broadcasted_iota(jnp.int32, (size, bq), 1) >= lax.broadcasted_iota(jnp.int32, (size, bq), 0)
        scores = [dot(k_ref[here, heads(i)], q_ref[:, heads(h)], 1, 1) for i, h in pieces]
        dps = [dot(v_ref[here, heads(i)], do_ref[:, heads(h)], 1, 1) for i, h in pieces]
        for (i, h), s, dp in zip(pieces, scores, dps):
            p = jnp.exp2(s * e - lse_ref[h : h + 1, :] * LOG2E)
            if masked:
                p = jnp.where(ok, p, 0.0)
            ds = (p * (dp - d_s[h : h + 1, :])).astype(bf16)
            dv_s[i, here, :] += dot(p.astype(bf16), do_ref[:, heads(h)])
            dk_s[i, here, :] += dot(ds, q_ref[:, heads(h)])
            dq_s[h] += dot(kT_s[i, :, here], ds)

    n = lax.div(iq * bq, bk)
    lax.fori_loop(0, n, lambda j, _: block(pl.multiple_of(j * bk, bk), bk, False), None)
    for r in range(1, bk // bq):

        @pl.when(lax.rem(iq, bk // bq) >= r)
        def _():
            block(pl.multiple_of(n * bk + (r - 1) * bq, bq), bq, False)

    block(pl.multiple_of(iq * bq, bq), bq, True)
    for _, h in pieces:
        d = (dq_s[h] * scale).T.astype(bf16).astype(f32)
        dq_ref[:, heads(h)] = turn(d, cos_ref[...], -sin_ref[...]).astype(bf16)

    now = pl.ds(pl.multiple_of(iq * bq, bq), bq)
    for i in range(kv):
        dkv_ref[:, heads(i)] = turn((dk_s[i, now, :] * scale).astype(bf16).astype(f32), cos_ref[...], -sin_ref[...]).astype(bf16)
        dkv_ref[:, heads(kv + i)] = dv_s[i, now, :].astype(bf16)
    if deeper:
        n = kv * HEAD
        by_a = dot(dq_ref[...], wq_ref[0], 1, 1) + dot(dkv_ref[:, :n], wk_ref[0], 1, 1) + dot(dkv_ref[:, n:], wv_ref[0], 1, 1)
        dh = (dh1_ref[...].astype(f32) + norm_back(h_ref[...], by_a.astype(bf16).astype(f32))).astype(bf16)
        dh_ref[...] = dh
        dhT_ref[...] = dh.T

    @pl.when(step == 0)
    def _():
        for c in parts(0):
            c.wait()
        for m in range(3):
            for n in range(2):
                two_s[m, n] = add(part_s[n, m, 0], part_s[n, m, 1]).astype(bf16)

    @pl.when(step == steps // 2 - 1)
    def _():
        for c in parts(1):
            c.wait()
        for m in range(3):
            twos[m].wait_recv()
            three_s[m] = add(part_s[0, m, 0], part_s[0, m, 1], got_two[m, 0]).astype(bf16)

    @pl.when(step == steps - 1)
    def _():
        total = 0.0
        for m in range(3):
            threes[m].wait_recv()
            own = add(part_s[1, m, 0], part_s[1, m, 1], got_two[m, 1], got_three[m]).astype(bf16)
            (gate_ref, up_ref, down_ref)[m][...] = own.T if m == 2 else own
            total += jnp.sum(jnp.square(own.astype(f32)))
        square_ref[...] = jnp.full(square_ref.shape, total, f32)
        for c in twos + threes:
            c.wait_send()


def attn_back(number, q, k, v, oT, do, lse, cos, sin, mine, came, deeper=None, bq=256, bk=512):
    t, w = q.shape
    kv, h = k.shape[1] // HEAD, w // HEAD
    d, bf = mine.shape[2:]
    steps = t // bq
    rows = lambda w: pl.BlockSpec((bq, w), lambda i: (steps - 1 - i, 0))
    cols = lambda w: pl.BlockSpec((w, bq), lambda i: (0, steps - 1 - i))
    hbm = pl.BlockSpec(memory_space=pl.ANY)
    dma = pltpu.SemaphoreType.DMA
    like = lambda *shape, dtype=bf16: jax.ShapeDtypeStruct(shape, dtype)
    more = deeper or ()
    sums = (kv, t, HEAD)
    return pl.pallas_call(
        functools.partial(_attn_back, kv=kv, g=h // kv, bq=bq, bk=bk, scale=HEAD**-0.5, deeper=deeper is not None),
        grid=(steps,),
        in_specs=[rows(w), once(k.shape), once(v.shape), cols(w), rows(w), cols(h), rows(HEAD), rows(HEAD)]
        + [once((1, *x.shape[1:]), (number, 0, 0)) for x in more[:3]] + [rows(d)] * len(more[3:]) + [hbm, hbm],
        out_specs=[rows(w), rows(2 * kv * HEAD), once((d, bf)), once((d, bf)), once((bf, d)), once((8, 128))] + ([rows(d), cols(d)] if more else []),
        out_shape=[like(t, w), like(t, 2 * kv * HEAD), like(d, bf), like(d, bf), like(bf, d), like(8, 128, dtype=f32)] + ([like(t, d), like(d, t)] if more else []),
        scratch_shapes=[pltpu.VMEM((h, HEAD, bq), f32), pltpu.VMEM(sums, f32), pltpu.VMEM(sums, f32), pltpu.VMEM((kv, HEAD, t), bf16),
                        pltpu.VMEM((h, bq), f32), pltpu.VMEM((2, 3, 2, d, bf), bf16),
                        pltpu.VMEM((3, 2, d, bf), bf16), pltpu.VMEM((3, 2, d, bf), bf16), pltpu.VMEM((3, d, bf), bf16), pltpu.VMEM((3, d, bf), bf16),
                        dma((2, 3, 2)), dma((3,)), dma((3,)), dma((3,)), dma((3,))],
        compiler_params=pltpu.CompilerParams(dimension_semantics=("arbitrary",), vmem_limit_bytes=VMEM,
                                             collective_id=3 + number, has_side_effects=True),
        cost_estimate=cost(8 * t * t * w, 12 * t * w),
        name=f"attn_back_{number}",
    )(q, k, v, oT, do, lse, cos, sin, *more, mine, came)


def gated(g):
    s = 1 / (1 + jnp.exp(-g))
    return s, g * s


def _mlp(b_ref, h1_ref, wg_ref, wu_ref, wd_ref, h2_ref, act_ref, by_g_ref, by_u_ref, acc_s, *, bm):
    j = pl.program_id(0)
    t = b_ref.shape[0]

    @pl.when(j == 0)
    def _():
        acc_s[...] = jnp.zeros_like(acc_s)

    rows = [pl.ds(i * bm, bm) for i in range(t // bm)]
    for i, r in enumerate(rows):
        g, u = dot(b_ref[r, :], wg_ref[0]), dot(b_ref[r, :], wu_ref[0])
        s, silu = gated(g)
        act_ref[0, r, :] = (silu * u).astype(bf16)
        by_g_ref[0, r, :] = u * (s * (1 + g * (1 - s)))
        by_u_ref[0, r, :] = silu
    for r in rows:
        acc_s[r, :] += dot(act_ref[0, r, :], wd_ref[0])

    @pl.when(j == pl.num_programs(0) - 1)
    def _():
        h2_ref[...] = (h1_ref[...].astype(f32) + acc_s[...].astype(bf16).astype(f32)).astype(bf16)


def mlp(number, b, h1, wg, wu, wd, bf=256, bm=512):
    t, d = b.shape
    n = wg.shape[2] // bf
    col = pl.BlockSpec((1, d, bf), lambda j: (number, 0, j))
    kept = pl.BlockSpec((1, t, bf), lambda j: (j, 0, 0))
    return pl.pallas_call(
        functools.partial(_mlp, bm=bm),
        grid=(n,),
        in_specs=[once((t, d)), once((t, d)), col, col, pl.BlockSpec((1, bf, d), lambda j: (number, j, 0))],
        out_specs=[once((t, d)), kept, kept, kept],
        out_shape=[jax.ShapeDtypeStruct((t, d), bf16), jax.ShapeDtypeStruct((n, t, bf), bf16)] + [jax.ShapeDtypeStruct((n, t, bf), f32)] * 2,
        scratch_shapes=[pltpu.VMEM((t, d), f32)],
        compiler_params=params("arbitrary"),
        cost_estimate=cost(6 * t * d * n * bf, 8 * t * n * bf),
        name=f"mlp_{number}",
    )(b, h1, wg, wu, wd)


def block_of(i, me):
    slot = lax.rem(3 * (7 - lax.rem(i, 8)), 8) * 2 + 1 - lax.div(i, 8)
    return sum(lax.rem(bit(slot, k) + bit(me, k), 2) * 2**k for k in range(4))


AXES = ((4, 3), (2, 2), (1, 1))


def chip_slot(k):
    return 3 * (7 - k) % 8 if isinstance(k, int) else lax.rem(3 * (7 - k), 8)


def _gated_back(*refs, stored, bm, deep):
    it = iter(refs)
    b_hbm = None if stored else next(it)
    bT_hbm, dh_hbm, dhT_hbm, h1_hbm, wo_ref, wg_ref, wu_ref, wd_ref = (next(it) for _ in range(8))
    act_ref, by_g_ref, by_u_ref = (next(it) for _ in range(3)) if stored else (None, None, None)
    dh1_hbm, do_hbm, mine, came, core_in = (next(it) for _ in range(5))
    b_s, act_s = (None, None) if stored else (next(it), next(it))
    (acc_s, bT_s, dh_s, dhT_s, h1_s, dgu_s, wgu_s, term_s, recv_s, load_sem, back_sem, core_send, core_recv, out_send, out_recv,
     keep_sem, recv_sem) = (next(it) for _ in range(17))
    i, me = pl.program_id(0), lax.axis_index("dp")
    t, bf = dgu_s.shape[0], dgu_s.shape[1] // 2

    def to_core(k):
        return pltpu.make_async_remote_copy(term_s.at[lax.rem(k, deep)], core_in.at[k], core_send.at[k], core_recv.at[k],
                                            device_id={"dp": flip(me, 0)}, device_id_type=pl.DeviceIdType.MESH)

    def to_chip(m, k):
        slot, (half, axis) = chip_slot(k), AXES[m]
        return pltpu.make_async_remote_copy(term_s.at[lax.rem(k + 8, deep), m], came.at[m, slot - half], out_send.at[m, k], out_recv.at[m, slot - half],
                                            device_id={"dp": flip(me, axis)}, device_id_type=pl.DeviceIdType.MESH)

    def keep(m, k):
        return pltpu.make_async_copy(term_s.at[lax.rem(k + 8, deep), m], mine.at[m, chip_slot(k)], keep_sem.at[m, k])

    def move(k, act):
        @pl.when(k < 8)
        def _():
            act(to_core(k))

        @pl.when(k >= 8)
        def _():
            for m in range(3):
                out = lax.rem(lax.div(chip_slot(k - 8), AXES[m][0]), 2) == 1

                @pl.when(out)
                def _():
                    act(to_chip(m, k - 8))

                @pl.when(jnp.logical_not(out))
                def _():
                    act(keep(m, k - 8))

    def start(c):
        c.start()

    def finish(c):
        (c.wait_send if hasattr(c, "wait_send") and c.is_remote else c.wait)()

    loads = [pltpu.make_async_copy(src, dst, load_sem.at[n]) for n, (src, dst) in enumerate(
        [(dh_hbm, dh_s)] + ([] if stored else [(b_hbm, b_s)]) + [(bT_hbm, bT_s), (dhT_hbm, dhT_s)])]
    first = 1 if stored else 2

    @pl.when(i == 0)
    def _():
        for c in loads:
            c.start()
        acc_s[...] = jnp.zeros_like(acc_s)
        recv_s[...] = jnp.zeros_like(recv_s)
        barrier = pltpu.get_barrier_semaphore()
        for axis in range(4):
            pl.semaphore_signal(barrier, inc=1, device_id={"dp": flip(me, axis)}, device_id_type=pl.DeviceIdType.MESH)
        pl.semaphore_wait(barrier, 4)
        for c in loads[:first]:
            c.wait()

    @pl.when(i >= 1)
    def _():
        move(i - 1, start)

    landed = pltpu.make_async_copy(core_in.at[lax.rem(i, 8)], recv_s, recv_sem.at[0])

    @pl.when(i >= 8)
    def _():
        to_core(i - 8).wait_recv()
        landed.start()

    wgu_s[:, :bf] = wg_ref[0]
    wgu_s[:, bf:] = wu_ref[0]
    rows = [pl.ds(r * bm, bm) for r in range(t // bm)]
    for r in rows:
        da = dot(dh_s[r, :], wd_ref[0], 1, 1).astype(bf16).astype(f32)
        if stored:
            by_g, by_u = by_g_ref[0, r, :], by_u_ref[0, r, :]
        else:
            gu = dot(b_s[r, :], wgu_s[...])
            g, u = gu[:, :bf], gu[:, bf:]
            s, by_u = gated(g)
            by_g = u * (s * (1 + g * (1 - s)))
            act_s[r, :] = (by_u * u).astype(bf16)
        dgu_s[r, bf:] = (da * by_u).astype(bf16)
        dgu_s[r, :bf] = (da * by_g).astype(bf16)
    for r in rows:
        acc_s[r, :] += dot(dgu_s[r, :], wgu_s[...], 1, 1)

    @pl.when(i == 0)
    def _():
        for c in loads[first:]:
            c.wait()

    @pl.when(i >= deep)
    def _():
        move(i - deep, finish)

    @pl.when(i >= 8)
    def _():
        landed.wait()

    place = lax.rem(i, deep)
    dgu = dot(bT_s[...], dgu_s[...])
    for m, term in enumerate((dgu[:, :bf], dgu[:, bf:], dot(dhT_s[...], act_ref[0] if stored else act_s[...]))):
        term_s[place, m] = (term + recv_s[m].astype(f32)).astype(bf16)

    @pl.when(i == 15)
    def _():
        for m in range(3):
            keep(m, 7).start()
        chunks = [pl.ds(n * 256, 256) for n in range(t // 256)]
        loaded = [pltpu.make_async_copy(h1_hbm.at[r], h1_s.at[n % 4], back_sem.at[0, n]) for n, r in enumerate(chunks)]
        gone = [pltpu.make_async_copy(h1_s.at[n % 4], dh1_hbm.at[r], back_sem.at[1, n]) for n, r in enumerate(chunks)]
        back = [pltpu.make_async_copy(dh_s.at[r], do_hbm.at[r], back_sem.at[2, n]) for n, r in enumerate(chunks)]
        for c in loaded[:4]:
            c.start()
        for n, r in enumerate(chunks):
            by_b = acc_s[r, :].astype(bf16).astype(f32)
            loaded[n].wait()
            dh1 = (dh_s[r, :].astype(f32) + norm_back(h1_s[n % 4], by_b)).astype(bf16)
            h1_s[n % 4] = dh1
            gone[n].start()
            dh_s[r, :] = dot(dh1, wo_ref[0], 1, 1).astype(bf16)
            back[n].start()
            if 1 <= n < len(chunks) - 3:
                gone[n - 1].wait()
                loaded[n + 3].start()
        for m in range(3):
            for k in range(8):
                out = chip_slot(k) // AXES[m][0] % 2 == 1
                if out:
                    to_chip(m, k).wait_recv()
                if k > 7 - deep:
                    to_chip(m, k).wait_send() if out else keep(m, k).wait()
        for c in gone[len(chunks) - 4 :] + back:
            c.wait()


def gated_back(number, bT, dh, dhT, h1, wg, wu, wd, wo, b=None, kept=None, bf=256, bm=512, deep=3):
    d, t = bT.shape
    stored = kept is not None
    col = pl.BlockSpec((1, d, bf), lambda i: (number, 0, block_of(i, lax.axis_index("dp"))))
    held = pl.BlockSpec((1, t, bf), lambda i: (block_of(i, lax.axis_index("dp")), 0, 0))
    hbm = pl.BlockSpec(memory_space=pl.ANY)
    given = ([] if stored else [b]) + [bT, dh, dhT, h1, wo, wg, wu, wd] + (list(kept) if stored else [])
    specs = [hbm] * (4 if stored else 5) + [once((1, *wo.shape[1:]), (number, 0, 0)), col, col]
    specs += [pl.BlockSpec((1, bf, d), lambda i: (number, block_of(i, lax.axis_index("dp")), 0))] + ([held] * 3 if stored else [])
    dma = pltpu.SemaphoreType.DMA
    got = pl.pallas_call(
        functools.partial(_gated_back, stored=stored, bm=bm, deep=deep),
        grid=(16,),
        in_specs=specs,
        out_specs=[hbm] * 5,
        out_shape=[jax.ShapeDtypeStruct((t, d), bf16), jax.ShapeDtypeStruct((t, wo.shape[1]), bf16)]
        + [jax.ShapeDtypeStruct((3, 8, d, bf), bf16)] * 2 + [jax.ShapeDtypeStruct((8, 3, d, bf), bf16)],
        scratch_shapes=([] if stored else [pltpu.VMEM((t, d), bf16), pltpu.VMEM((t, bf), bf16)])
        + [pltpu.VMEM((t, d), f32), pltpu.VMEM((d, t), bf16), pltpu.VMEM((t, d), bf16), pltpu.VMEM((d, t), bf16), pltpu.VMEM((4, 256, d), bf16),
           pltpu.VMEM((t, 2 * bf), bf16), pltpu.VMEM((d, 2 * bf), bf16), pltpu.VMEM((deep, 3, d, bf), bf16),
           pltpu.VMEM((3, d, bf), bf16), dma((4,)), dma((3, t // 256)), dma((8,)), dma((8,)), dma((3, 8)), dma((3, 8)), dma((3, 8)), dma((1,))],
        compiler_params=pltpu.CompilerParams(dimension_semantics=("arbitrary",), vmem_limit_bytes=VMEM, collective_id=1 + number, has_side_effects=True),
        cost_estimate=cost(2 * t * d * bf * 16 * (6 if stored else 8), 8 * t * bf * 16),
        name=f"gated_back_{number}",
    )(*given)
    return got[:4]


def _attn_sums(*refs, count):
    layers = [refs[5 * n : 5 * n + 5] for n in range(2)]
    square_ref, square_too_ref, own_ref, factor_ref = refs[10:14]
    (aT_s, oT_s, right_s, term_s, from_core, sum_s, keep_s, one_s, got_one, two_s, got_two, three_s, got_three, sq_s, got_sq,
     load_sem, core_send, core_recv, send_sem, recv_sem, sq_send, sq_recv) = refs[14:]
    step, me = pl.program_id(0), lax.axis_index("dp")
    chip, core = lax.div(me, 2), lax.rem(me, 2)
    to = lambda axis: dict(device_id={"dp": flip(me, axis)}, device_id_type=pl.DeviceIdType.MESH)
    d, w = sum_s.shape
    third, high = w // 3, d // 8
    q, n = layers[0][1].shape[1] // 2, layers[0][2].shape[1] // 4

    def loads(at):
        aT, dq, dkv, oT, dh1 = layers[at // 2]
        half = lax.rem(core + 1 + at, 2)
        columns = lambda first, wide: pl.ds(pl.multiple_of(first + half * wide, 128), wide)
        ins = [(dq.at[:, columns(0, q)], right_s.at[:, pl.ds(0, q)]), (dkv.at[:, columns(0, n)], right_s.at[:, pl.ds(q, n)]),
               (dkv.at[:, columns(2 * n, n)], right_s.at[:, pl.ds(q + n, n)])] + ([(aT, aT_s)] if at % 2 == 0 else [])
        outs = [(dh1.at[:, columns(0, q)], right_s.at[:, pl.ds(q + 2 * n, q)])] + ([(oT, oT_s)] if at % 2 == 0 else [])
        sem = iter(range(6))
        return [[pltpu.make_async_copy(a, b, load_sem.at[at, next(sem)]) for a, b in some] for some in (ins, outs)]

    def each(act):
        for at in range(4):
            pl.when(step == at)(functools.partial(act, at))

    def go(copies):
        for c in copies:
            c.start()

    def arrive(copies):
        for c in copies:
            c.wait()

    def to_core(layer):
        return pltpu.make_async_remote_copy(term_s, from_core.at[layer], core_send.at[layer], core_recv.at[layer], **to(0))

    def exchange(layer, phase):
        src, dst = ((one_s, got_one), (two_s, got_two), (three_s, got_three))[phase]
        return [pltpu.make_async_remote_copy(src.at[m], dst.at[layer, m], send_sem.at[layer, phase, m], recv_sem.at[layer, phase, m],
                                             **to(PLACE[TURN[m][phase]])) for m in range(3)]

    def part(layer, m, slot):
        rows = pl.ds(pl.multiple_of(flips(chip, slot) * high, high), high)
        cols = slice(m * third, (m + 1) * third)
        return add(sum_s[rows, cols], from_core[layer, rows, cols])

    def begin(layer):
        to_core(layer).wait()
        for m, (a, b, c) in enumerate(TURN):
            for at, rest in enumerate((b | c, b, c, 0)):
                one_s[m, at] = part(layer, m, a | rest).astype(bf16)
                keep_s[layer, m, at] = part(layer, m, rest)
        go(exchange(layer, 0))

    def second(layer):
        for m, e in enumerate(exchange(layer, 0)):
            e.wait()
            for at in range(2):
                two_s[m, at] = add(keep_s[layer, m, at], got_one[layer, m, at]).astype(bf16)
        go(exchange(layer, 1))

    def last(layer):
        for m, e in enumerate(exchange(layer, 1)):
            e.wait()
            three_s[m] = add(keep_s[layer, m, 2], got_one[layer, m, 2], got_two[layer, m, 0]).astype(bf16)
        go(exchange(layer, 2))

    def end(layer):
        total = 0.0
        for m, e in enumerate(exchange(layer, 2)):
            e.wait()
            own = add(keep_s[layer, m, 3], got_one[layer, m, 3], got_two[layer, m, 1], got_three[layer, m]).astype(bf16)
            own_ref[layer, :, m * third : (m + 1) * third] = own
            total += jnp.sum(jnp.square(own.astype(f32)))
        return total

    @pl.when(step == 0)
    def _():
        for some in loads(0):
            go(some)
        barrier = pltpu.get_barrier_semaphore()
        pl.semaphore_signal(barrier, inc=1, **to(0))
        for n in range(1, 8):
            pl.semaphore_signal(barrier, inc=1, device_id={"dp": flips(me, 2 * n)}, device_id_type=pl.DeviceIdType.MESH)
        pl.semaphore_wait(barrier, 8)

    @pl.when(step == 1)
    def _():
        to_core(0).start()

    @pl.when(step == 3)
    def _():
        to_core(1).start()

    each(lambda at: arrive(loads(at)[0]))
    sum_s[:, : q + 2 * n] = dot(aT_s[...], right_s[:, : q + 2 * n])
    each(lambda at: go(loads(at + 1)[0]) if at < 3 else None)

    @pl.when(step == 3)
    def _():
        second(0)

    each(lambda at: arrive(loads(at)[1]))
    sum_s[:, q + 2 * n :] = dot(oT_s[...], right_s[:, q + 2 * n :])
    each(lambda at: go(loads(at + 1)[1]) if at < 3 else None)

    @pl.when(lax.rem(step, 2) == 0)
    def _():
        term_s[...] = sum_s[...].astype(bf16)

    @pl.when(step == 1)
    def _():
        begin(0)

    @pl.when(step == 3)
    def _():
        last(0)
        begin(1)
        own_square = end(0)
        second(1)
        last(1)
        own_square += end(1)
        sq_s[0] = square_ref[...] + square_too_ref[...] + own_square
        c = pltpu.make_async_remote_copy(sq_s.at[0], got_sq.at[0], sq_send.at[0], sq_recv.at[0], **to(0))
        c.start()
        c.wait()
        sq_s[1] = sq_s[0] + got_sq[0]
        cs = [pltpu.make_async_remote_copy(sq_s.at[1], got_sq.at[n], sq_send.at[n], sq_recv.at[n], device_id={"dp": flips(me, 2 * n)},
                                           device_id_type=pl.DeviceIdType.MESH) for n in range(1, 8)]
        go(cs)
        arrive(cs)
        got_sq[0] = sq_s[1]
        total = got_sq[chip]
        for n in range(1, 8):
            total = total + got_sq[flips(chip, n)]
        factor_ref[...] = jnp.minimum(1.0, 0.5 * lax.rsqrt(total / count + 1e-30))


def attn_sums(layers, squares, count):
    aT, dq, dkv = layers[0][:3]
    d, t = aT.shape
    w = dq.shape[1] + dkv.shape[1] // 2 + layers[0][4].shape[1] // 2 - dq.shape[1] // 2
    third, high = w // 3, d // 8
    hbm = pl.BlockSpec(memory_space=pl.ANY)
    dma = pltpu.SemaphoreType.DMA
    vm = lambda *shape, dtype=bf16: pltpu.VMEM(shape, dtype)
    return pl.pallas_call(
        functools.partial(_attn_sums, count=count),
        grid=(4,),
        in_specs=[hbm] * 10 + [once((8, 128))] * 2,
        out_specs=[once((2, high, w)), once((8, 128))],
        out_shape=[jax.ShapeDtypeStruct((2, high, w), bf16), jax.ShapeDtypeStruct((8, 128), f32)],
        scratch_shapes=[vm(d, t), vm(d, t), vm(t, w), vm(d, w), vm(2, d, w), vm(d, w, dtype=f32), vm(2, 3, 4, high, third, dtype=f32),
                        vm(3, 4, high, third), vm(2, 3, 4, high, third), vm(3, 2, high, third), vm(2, 3, 2, high, third), vm(3, high, third),
                        vm(2, 3, high, third), vm(2, 8, 128, dtype=f32), vm(8, 8, 128, dtype=f32),
                        dma((4, 6)), dma((2,)), dma((2,)), dma((2, 3, 3)), dma((2, 3, 3)), dma((8,)), dma((8,))],
        compiler_params=pltpu.CompilerParams(dimension_semantics=("arbitrary",), vmem_limit_bytes=VMEM, collective_id=5, has_side_effects=True),
        cost_estimate=cost(8 * t * d * w, 32 * t * d),
        name="attn_sums",
    )(*layers[0], *layers[1], *squares)


def _adamw(factor_ref, *refs, widths, form, old):
    k = len(widths)
    gs = k if form != "cores" else 1
    ins, gs, outs = refs[: 3 * k], refs[3 * k : 3 * k + gs], refs[3 * k + gs + old * 3 * k :]
    factor = factor_ref[:1, :1]

    def one(a, cols, g):
        w_ref, m_ref, v_ref = ins[3 * a : 3 * a + 3]
        nw_ref, nm_ref, nv_ref = outs[3 * a : 3 * a + 3]
        g = g.astype(f32) * factor
        m = 0.9 * m_ref[0, :, cols] + 0.1 * g
        v = 0.95 * v_ref[0, :, cols] + 0.05 * g * g
        w = w_ref[0, :, cols].astype(f32)
        nm_ref[0, :, cols] = m
        nv_ref[0, :, cols] = v
        nw_ref[0, :, cols] = (w - 0.02 * (m * lax.rsqrt(v + 1e-8) + 0.1 * w)).astype(bf16)

    for a, width in enumerate(widths):
        if form == "cores":
            at = sum(widths[:a]) // 2
            for c in range(2):
                one(a, slice(c * width // 2, (c + 1) * width // 2), gs[0][0, c, 0, :, at : at + width // 2])
        elif len(gs[a].shape) == 3:
            n, wide = gs[a].shape[0], gs[a].shape[2]
            for c in range(n):
                one(a, slice(c * wide, (c + 1) * wide), gs[a][c])
        else:
            one(a, slice(None), gs[a][...])


def adamw(number, factor, arrays, gs, before=None, form="", rows=32):
    height = arrays[0][0].shape[1]
    widths = [a[0].shape[2] for a in arrays]
    given, specs, out_specs, out_shape = [factor], [once(factor.shape)], [], []
    for (w, m, v), width in zip(arrays, widths):
        block = pl.BlockSpec((1, rows, width), lambda i: (number, i, 0))
        given += [w, m, v]
        specs += [block] * 3
        out_specs += [block] * 3
        out_shape += [jax.ShapeDtypeStruct(w.shape, bf16), jax.ShapeDtypeStruct(m.shape, f32), jax.ShapeDtypeStruct(v.shape, f32)]
    for g, width in zip(gs, widths):
        g, at = g if isinstance(g, tuple) else (g, 0)
        given += [g]
        if form == "cores":
            per = g.shape[3] // rows
            specs += [pl.BlockSpec((1, 2, 1, rows, g.shape[4]), lambda i: (lax.div(i, per), 0, 1 - number, lax.rem(i, per), 0))]
        elif g.ndim == 3:
            specs += [pl.BlockSpec((g.shape[0], rows, g.shape[2]), lambda i: (0, i, 0))]
        else:
            specs += [pl.BlockSpec((rows, width), lambda i, at=at: (i, at))]
    alias = {}
    if before is not None:
        flat = [x for one in before for x in one]
        alias = {len(given) + i: i for i in range(len(flat))}
        given += flat
        specs += [pl.BlockSpec(memory_space=pl.ANY)] * len(flat)
    got = pl.pallas_call(
        functools.partial(_adamw, widths=widths, form=form, old=int(before is not None)),
        grid=(height // rows,),
        in_specs=specs,
        out_specs=out_specs,
        out_shape=out_shape,
        input_output_aliases=alias,
        compiler_params=params("arbitrary"),
        cost_estimate=cost(20 * height * sum(widths), 22 * height * sum(widths)),
        name=f"adamw_{number}_{len(arrays)}",
    )(*given)
    return [tuple(got[3 * a : 3 * a + 3]) for a in range(len(arrays))]


def solution(mesh):
    def step(x, dy, *arrays):
        weights, first, second = (dict(zip(NAMES, arrays[i : i + 7], strict=True)) for i in (0, 7, 14))
        wq, wk, wv, wo, wg, wu, wd = (weights[name] for name in NAMES)
        x, dy = x[0], dy[0]
        t, d = x.shape
        me = lax.axis_index("dp").astype(jnp.int32)
        half = HEAD // 2
        angle = jnp.arange(t, dtype=f32)[:, None] * THETA ** (-jnp.arange(half, dtype=f32) / half)
        cos = jnp.concatenate([jnp.cos(angle)] * 2, 1)
        sin = jnp.concatenate([-jnp.sin(angle), jnp.sin(angle)], 1)

        q0, k0, v0, aT0, dyT = qkv(0, x, wq, wk, wv, cos, sin, also=dy)
        o0, oT0, lse0 = attn(0, q0, k0, v0)
        h01, b0, bT0 = out(0, o0, wo, x)
        h1, *kept0 = mlp(0, b0, h01, wg, wu, wd)
        q1, k1, v1, aT1 = qkv(1, h1, wq, wk, wv, cos, sin)
        o1, oT1, lse1 = attn(1, q1, k1, v1)
        h11, b1, bT1 = out(1, o1, wo, h1)

        def gather(gate, up, down):
            return [lax.all_gather(gate, "dp"), lax.all_gather(up, "dp"), lax.all_gather(down, "dp", tiled=True)]

        after = lambda *xs: lax.optimization_barrier(xs)
        dh11, do1, mine, came = gated_back(1, bT1, dy, dyT, h11, wg, wu, wd, wo, b=b1)
        dq1, dkv1, *sums1, square1, dh, dhT = attn_back(1, q1, k1, v1, oT1, do1, lse1, cos, sin, mine, came, deeper=(wq, wk, wv, h1, dh11))
        gathered1 = gather(*sums1)
        dh01, do0, mine, came = gated_back(0, bT0, dh, dhT, h01, wg, wu, wd, wo, kept=kept0)
        do0, gathered1[0], gathered1[1] = after(do0, gathered1[0], gathered1[1])
        dq0, dkv0, *sums0, square0 = attn_back(0, q0, k0, v0, oT0, do0, lse0, cos, sin, mine, came)
        dq0, gathered1[2] = after(dq0, gathered1[2])
        squares = square1, square0
        part, factor = attn_sums(((aT1, dq1, dkv1, oT1, dh11), (aT0, dq0, dkv0, oT0, dh01)), squares, sum(w.size for w in weights.values()))
        rest = lax.all_gather(part, "dp").reshape(DEVICES // 2, 2, *part.shape)
        part, *sums0 = after(part, *sums0)
        gathered0 = gather(*sums0)

        of = lambda names: [(weights[name], first[name], second[name]) for name in names]
        new_attn = adamw(1, factor, of(NAMES[:4]), [rest], form="cores", rows=160)
        new_up = adamw(1, factor, of(NAMES[4:6]), gathered1[:2], rows=64)
        new_down = adamw(1, factor, of(NAMES[6:]), gathered1[2:], rows=512)
        new_up = [adamw(0, factor, of(NAMES[4 + n : 5 + n]), gathered0[n : n + 1], before=new_up[n : n + 1], rows=128)[0] for n in range(2)]
        new_down = adamw(0, factor, of(NAMES[6:]), gathered0[2:], before=new_down, rows=512)
        new_attn = adamw(0, factor, of(NAMES[:4]), [rest], before=new_attn, form="cores", rows=160)
        new = new_attn + new_up + new_down
        return tuple(n[which] for which in range(3) for n in new)

    states, all_of = P(("rep", "dp"), None, None), P(None, None, None)
    return jax.shard_map(
        step,
        mesh=mesh,
        in_specs=(states, states) + (all_of,) * 21,
        out_specs=(P("rep", None, None),) * 21,
        check_vma=False,
    )
```
